256 devices in a mesh: row: 16 (over y, x), col: 16 (over z, core).
Axes of the slice: x: 4, y: 4, z: 8, core: 2. Of those that a mesh axis runs over, the one named last changes fastest.
Arguments:
- depth: float32 [1024, 8192], P('row', 'col'), may hold values from 0 to 1
- rainfall: float32 [1024, 8192], P('row', 'col'), may hold values from 0.05 to 0.5
- conveyance: float32 [1024, 8192], P('row', 'col'), may hold values from 0.2 to 5
- flow_dir: int32 [1024, 8192], P('row', 'col'), may hold values from 0 to 7, as said below
- outlet: int32 [1024, 8192], P('row', 'col'), may hold values 0 or 1
Outputs:
- new_depth: float32 [1024, 8192], P('row', 'col')
- discharge: float32 [1024, 8192], P('row', 'col')
The draws below stay inside these ranges and needn't reach their ends.
Inputs may be any that keep to these rules, and one draw needn't show every extreme that they name: `flow_dir`: each cell's code is 0 to 7.
All inputs are finite; a program needn't handle non-finite values. No bound on the sum of `outlet` on one device may be relied on, other than what follows from the above.
Results may differ from the reference program's by a relative error of at most 0.00002.
Values sent between devices are 32-bit elements; how exact they have to be, the bound alone decides.
A program may use at most 64 MiB of HBM per device.

```python
import math
import jax
import jax.numpy as jnp

SUBSTEPS = 3
PASSES = 64
NR = 1024
NC = 8192


def draw_flow_dir(key, part):
    first = jax.random.fold_in(key, 11)
    second = jax.random.fold_in(key, 12)
    third = jax.random.fold_in(key, 13)
    picker = jax.random.randint(first, (NR, NC), 0, 10)
    drift = jax.random.randint(second, (NR, NC), 0, 3)
    anyway = jax.random.randint(third, (NR, NC), 0, 8)
    return jnp.where(picker < 7, drift, anyway).astype(jnp.int32)


def plant(array, key, low, top_value):
    longest = array.shape.index(max(array.shape))
    spots = []
    for shift in (0, 1):
        where = [jax.random.randint(jax.random.fold_in(key, axis), (), 0, length) for axis, length in enumerate(array.shape)]
        where[longest] = (where[longest] + shift) % array.shape[longest]
        spots.append(tuple(where))
    return array.at[spots[0]].set(low).at[spots[1]].set(top_value)


def levels(own_key, extent, split, low, largest):
    def one(axis_at, blocks):
        draws = jax.random.uniform(jax.random.fold_in(jax.random.fold_in(own_key, 6), axis_at), (blocks,), jnp.float32, low / len(split), largest / len(split))
        return jnp.repeat(jnp.exp(draws), extent[axis_at] // blocks).reshape((-1,) + (1,) * (len(extent) - axis_at - 1))

    gain = one(*split[0])
    for cut in split[1:]:
        gain = gain * one(*cut)
    return gain


def setup_inputs(seed: int = 0) -> dict:
    arg_keys = jax.random.split(jax.random.key(seed), 6)
    depth = jnp.clip(1.0 * jax.random.uniform(arg_keys[0], (NR, NC), jnp.float32) ** levels(arg_keys[0], (NR, NC), ((0, 16), (1, 16)), -0.2, 0.2), 0.0, 1.0)
    rainfall = jnp.clip(jnp.exp(math.log(0.5) - 2.3025851 * jax.random.uniform(arg_keys[1], (NR, NC), jnp.float32) ** levels(arg_keys[1], (NR, NC), ((0, 16), (1, 16)), -0.2, 0.2)), 0.05, 0.5)
    conveyance = jnp.clip(jnp.exp(math.log(5.0) - 3.218876 * jax.random.uniform(arg_keys[2], (NR, NC), jnp.float32) ** levels(arg_keys[2], (NR, NC), ((0, 16), (1, 16)), -0.2, 0.2)), 0.2, 5.0)
    flow_dir = draw_flow_dir(jax.random.fold_in(arg_keys[5], 71), 0)
    outlet = plant((jax.random.randint(arg_keys[4], (NR, NC), 0, 32) < 1).astype(jnp.int32), jax.random.fold_in(arg_keys[4], 1), 0, 1)
    return dict(depth=depth, rainfall=rainfall, conveyance=conveyance, flow_dir=flow_dir, outlet=outlet)


OFFSETS = ((0, 1), (1, 1), (1, 0), (1, -1), (0, -1), (-1, -1), (-1, 0), (-1, 1))


def inflow(sent, route):
    sent_pad = jnp.pad(sent, 1)
    route_pad = jnp.pad(route, 1)
    rows, cols = sent.shape
    total = jnp.zeros((rows, cols), jnp.float32)
    for k, (di, dj) in enumerate(OFFSETS):
        source = sent_pad[1 - di:1 - di + rows, 1 - dj:1 - dj + cols]
        target = route_pad[1 - di:1 - di + rows, 1 - dj:1 - dj + cols]
        total = total + jnp.where(target == k + 1, source, jnp.float32(0.0))
    return total


def reference(depth, rainfall, conveyance, flow_dir, outlet):
    route = jnp.where(outlet == 1, 0, flow_dir + 1).astype(jnp.int32)
    length = jnp.where(flow_dir % 2 == 1, jnp.float32(0.70710678), jnp.float32(1.0))
    level = depth
    for step in range(SUBSTEPS):
        factor = conveyance * length * jnp.power(level, jnp.float32(2.0 / 3.0))
        share = factor / (1.0 + factor)
        out = level * share
        sent = jnp.where(route > 0, out, jnp.float32(0.0))
        level = level + rainfall - out + inflow(sent, route)

    def one_pass(index, acc):
        sent = jnp.where(route > 0, acc, jnp.float32(0.0))
        return level + inflow(sent, route)

    acc = jax.lax.fori_loop(0, PASSES, one_pass, level)
    return level, jnp.log(1.0 + acc)
```

```python
import functools

import jax
import jax.numpy as jnp
from jax import lax
from jax.experimental import pallas as pl
from jax.experimental.pallas import tpu as pltpu
from jax.sharding import PartitionSpec as P

SUBSTEPS = 3
PASSES = 64
MARGIN = 32
NEAR = 8
LANES = 128
MESH = pl.DeviceIdType.MESH
OFFSETS = ((0, 1), (1, 1), (1, 0), (1, -1), (0, -1), (-1, -1), (-1, 0), (-1, 1))
SIDES = ((-1, 0), (1, 0), (0, -1), (0, 1), (-1, -1), (-1, 1), (1, -1), (1, 1))


def kernel(
    rows, cols, nrow, ncol,
    depth, rainfall, conveyance, flow_dir, outlet, new_depth, discharge,
    raw, raw_side, flow, out_of, route, route_side, level, level_side, sent, masks, acc, far,
    in_sem, out_sem, raw_ssem, raw_rsem, route_ssem, route_rsem, level_ssem, level_rsem, far_ssem, far_rsem,
):
    strips = cols // LANES
    total = strips + 1
    top = MARGIN + 8
    end = top + rows
    me_r, me_c = lax.axis_index("row"), lax.axis_index("col")
    lane = lax.broadcasted_iota(jnp.int32, (8, LANES), 1)
    zero = jnp.zeros((8, LANES), jnp.float32)

    def present(dr, dc):
        r, c = me_r + dr, me_c + dc
        return (r >= 0) & (r < nrow) & (c >= 0) & (c < ncol)

    loads = []
    for a, (source, target) in enumerate((
        (flow_dir, flow), (outlet, out_of), (depth, raw.at[0]), (rainfall, raw.at[1]), (conveyance, raw.at[2]),
    )):
        for w in range(strips):
            rows_at = pl.ds(0, rows) if a < 2 else pl.ds(top, rows)
            loads.append(pltpu.make_async_copy(
                source.at[:, pl.ds(w * LANES, LANES)], target.at[w, rows_at, :], in_sem.at[a, w]))
    for load in loads:
        load.start()

    def clear(ref, first, last):
        for r in range(first, last, 8):
            ref[pl.ds(r, 8), :] = zero

    for w in range(strips):
        for a in range(3):
            clear(raw.at[a, w], top - NEAR, top)
            clear(raw.at[a, w], end, end + NEAR)
        for ref in (route, level):
            clear(ref.at[w], top - MARGIN, top)
            clear(ref.at[w], end, end + MARGIN)
    for side in range(2):
        for a in range(3):
            clear(raw_side.at[side, a], top - NEAR, end + NEAR)
        for ref in (route_side, level_side):
            clear(ref.at[side], top - MARGIN, end + MARGIN)
        for w in range(total):
            clear(far.at[side, w], 0, MARGIN)

    barrier = pltpu.get_barrier_semaphore()
    neighbours = jnp.int32(0)
    for dr, dc in SIDES:
        here = present(dr, dc)
        neighbours = neighbours + here.astype(jnp.int32)

        @pl.when(here)
        def _():
            pl.semaphore_signal(barrier, inc=1, device_id=(me_r + dr, me_c + dc), device_id_type=MESH)

    def copies(main, side, reach, ssem, rsem):
        made = []
        for d, (dr, dc) in enumerate(SIDES):
            if dr == 0:
                source, target = pl.ds(top, rows), pl.ds(top, rows)
            elif dr < 0:
                source, target = pl.ds(top, reach), pl.ds(end, reach)
            else:
                source, target = pl.ds(end - reach, reach), pl.ds(top - reach, reach)
            if dc == 0:
                src, dst = main(None, source), main(None, target)
            elif dc < 0:
                src, dst = main(0, source), side(1, target)
            else:
                src, dst = main(strips - 1, source), side(0, target)
            made.append(pltpu.make_async_remote_copy(
                src_ref=src, dst_ref=dst, send_sem=ssem.at[d], recv_sem=rsem.at[d],
                device_id=(me_r + dr, me_c + dc), device_id_type=MESH))
        return made

    def on_each(made, act, flip):
        for copy, (dr, dc) in zip(made, SIDES):
            @pl.when(present(-dr, -dc) if flip else present(dr, dc))
            def _():
                act(copy)

    def start_all(made):
        on_each(made, lambda copy: copy.start(), False)

    def arrive_all(made):
        on_each(made, lambda copy: copy.wait_recv(), True)

    def leave_all(made):
        on_each(made, lambda copy: copy.wait_send(), False)

    raw_copies = copies(
        lambda w, at: raw.at[:, pl.ds(0, strips), at, :] if w is None else raw.at[:, w, at, :],
        lambda s, at: raw_side.at[s, :, at, :], NEAR, raw_ssem, raw_rsem)
    route_copies = copies(
        lambda w, at: route.at[pl.ds(0, strips), at, :] if w is None else route.at[w, at, :],
        lambda s, at: route_side.at[s, at, :], MARGIN, route_ssem, route_rsem)
    level_copies = copies(
        lambda w, at: level.at[pl.ds(0, strips), at, :] if w is None else level.at[w, at, :],
        lambda s, at: level_side.at[s, at, :], MARGIN, level_ssem, level_rsem)

    for load in loads:
        load.wait()
    for w in range(strips):
        for r in range(0, rows, 8):
            at, here = pl.ds(r, 8), pl.ds(top + r, 8)
            code = flow[w, at, :]
            route[w, here, :] = jnp.where(out_of[w, at, :] == 1, 0, code + 1).astype(jnp.float32)
            length = jnp.where(code % 2 == 1, jnp.float32(0.70710678), jnp.float32(1.0))
            raw[2, w, here, :] = raw[2, w, here, :] * length

    pl.semaphore_wait(barrier, neighbours)
    start_all(raw_copies)
    start_all(route_copies)

    def merge(main, side, first, last):
        for r in range(first, last, 8):
            at = pl.ds(r, 8)
            main[strips, at, :] = jnp.where(lane < LANES // 2, side[1, at, :], side[0, at, :])

    arrive_all(raw_copies)
    arrive_all(route_copies)
    for a in range(3):
        merge(raw.at[a], raw_side.at[:, a], top - NEAR, end + NEAR)
    merge(route, route_side, top - MARGIN, end + MARGIN)

    def make_masks(first, last):
        for w in range(total):
            for r in range(first, last, 8):
                near = {di: route[w, pl.ds(r - di, 8), :] for di in (-1, 0, 1)}
                for k, (di, dj) in enumerate(OFFSETS):
                    masks[k, w, pl.ds(r, 8), :] = jnp.where(
                        near[di] == jnp.float32(k + 1), jnp.float32(1.0), jnp.float32(0.0))

    def inflow(source, base, r):
        east, west, still = [], [], []
        here = pl.ds(r, 8)
        for w in range(total):
            x = {di: source[w, pl.ds(r - di, 8), :] for di in (-1, 0, 1)}
            term = [masks[k, w, here, :] * x[di] for k, (di, _) in enumerate(OFFSETS)]
            east.append(term[0] + term[1] + term[7])
            west.append(term[3] + term[4] + term[5])
            still.append(base(w, here) + term[2] + term[6])
        east = [pltpu.roll(x, 1, 1) for x in east]
        west = [pltpu.roll(x, LANES - 1, 1) for x in west]
        return [
            still[w]
            + jnp.where(lane == 0, east[w - 1], east[w])
            + jnp.where(lane == LANES - 1, west[(w + 1) % total], west[w])
            for w in range(total)
        ]

    make_masks(top - NEAR, end + NEAR)
    for step in range(SUBSTEPS):
        held = raw.at[0] if step == 0 else acc.at[0]
        for w in range(total):
            for r in range(top - NEAR, end + NEAR, 8):
                at = pl.ds(r, 8)
                h = held[w, at, :]
                factor = raw[2, w, at, :] * jnp.exp(jnp.log(h) * jnp.float32(2.0 / 3.0))
                out = h * (factor / (1.0 + factor))
                sent[w, at, :] = out
                acc[0, w, at, :] = h + raw[1, w, at, :] - out
        target = acc.at[0] if step < SUBSTEPS - 1 else level
        for r in range(top - NEAR, end + NEAR, 8):
            if step == SUBSTEPS - 1 and not top <= r < end:
                continue
            new = inflow(sent, lambda w, at: acc[0, w, at, :], r)
            for w in range(total if step < SUBSTEPS - 1 else strips):
                target[w, pl.ds(r, 8), :] = new[w]

    start_all(level_copies)
    stores = [
        pltpu.make_async_copy(
            level.at[w, pl.ds(top, rows), :], new_depth.at[:, pl.ds(w * LANES, LANES)], out_sem.at[0, w])
        for w in range(strips)
    ]
    for store in stores:
        store.start()
    make_masks(top - MARGIN, top - NEAR)
    make_masks(end + NEAR, end + MARGIN)
    arrive_all(level_copies)
    merge(level, level_side, top - MARGIN, end + MARGIN)

    def one_pass(source, target, first, last):
        for r in range(first, last, 8):
            new = inflow(source, lambda w, at: level[w, at, :], r)
            for w in range(total):
                target[w, pl.ds(r, 8), :] = new[w]

    def segment(source):
        one_pass(source, acc.at[1], top - MARGIN, end + MARGIN)
        one_pass(acc.at[1], acc.at[0], top - MARGIN, end + MARGIN)
        for g in range(0, MARGIN, 8):
            def pair(_, carry):
                one_pass(acc.at[0], acc.at[1], top - MARGIN + g, end + MARGIN - g)
                one_pass(acc.at[1], acc.at[0], top - MARGIN + g, end + MARGIN - g)
                return carry

            lax.fori_loop(1 if g == 0 else 0, 4, pair, 0)

    segment(level)
    for seg in range(1, PASSES // MARGIN):
        up = pltpu.make_async_remote_copy(
            src_ref=acc.at[0, :, pl.ds(top, MARGIN), :], dst_ref=far.at[1], send_sem=far_ssem.at[seg, 0],
            recv_sem=far_rsem.at[seg, 0], device_id=(me_r - 1, me_c), device_id_type=MESH)
        down = pltpu.make_async_remote_copy(
            src_ref=acc.at[0, :, pl.ds(end - MARGIN, MARGIN), :], dst_ref=far.at[0], send_sem=far_ssem.at[seg, 1],
            recv_sem=far_rsem.at[seg, 1], device_id=(me_r + 1, me_c), device_id_type=MESH)
        has_up, has_down = present(-1, 0), present(1, 0)
        pl.when(has_up)(lambda: up.start())
        pl.when(has_down)(lambda: down.start())
        pl.when(has_down)(lambda: up.wait_recv())
        pl.when(has_up)(lambda: down.wait_recv())
        pl.when(has_up)(lambda: up.wait_send())
        pl.when(has_down)(lambda: down.wait_send())
        for w in range(total):
            for r in range(0, MARGIN, 8):
                acc[0, w, pl.ds(top - MARGIN + r, 8), :] = far[0, w, pl.ds(r, 8), :]
                acc[0, w, pl.ds(end + r, 8), :] = far[1, w, pl.ds(r, 8), :]
        segment(acc.at[0])

    for w in range(strips):
        for r in range(0, rows, 8):
            sent[w, pl.ds(top + r, 8), :] = jnp.log(1.0 + acc[0, w, pl.ds(top + r, 8), :])
    ends = [
        pltpu.make_async_copy(
            sent.at[w, pl.ds(top, rows), :], discharge.at[:, pl.ds(w * LANES, LANES)], out_sem.at[1, w])
        for w in range(strips)
    ]
    for store in ends:
        store.start()
    leave_all(raw_copies)
    leave_all(route_copies)
    leave_all(level_copies)
    for store in stores + ends:
        store.wait()


def solution(mesh):
    nrow, ncol = mesh.shape["row"], mesh.shape["col"]

    def on_device(depth, rainfall, conveyance, flow_dir, outlet):
        rows, cols = depth.shape
        strips = cols // LANES
        total = strips + 1
        high = rows + 2 * MARGIN + 16
        f32 = functools.partial(pltpu.VMEM, dtype=jnp.float32)
        dma = pltpu.SemaphoreType.DMA
        segments = PASSES // MARGIN
        return tuple(pl.pallas_call(
            functools.partial(kernel, rows, cols, nrow, ncol),
            out_shape=[jax.ShapeDtypeStruct((rows, cols), jnp.float32)] * 2,
            in_specs=[pl.BlockSpec(memory_space=pl.ANY)] * 5,
            out_specs=[pl.BlockSpec(memory_space=pl.ANY)] * 2,
            scratch_shapes=[
                f32((3, total, high, LANES)),
                f32((2, 3, high, LANES)),
                pltpu.VMEM((strips, rows, LANES), jnp.int32),
                pltpu.VMEM((strips, rows, LANES), jnp.int32),
                f32((total, high, LANES)),
                f32((2, high, LANES)),
                f32((total, high, LANES)),
                f32((2, high, LANES)),
                f32((total, high, LANES)),
                f32((8, total, high, LANES)),
                f32((2, total, high, LANES)),
                f32((2, total, MARGIN, LANES)),
                dma((5, strips)),
                dma((2, strips)),
                dma((8,)), dma((8,)), dma((8,)), dma((8,)), dma((8,)), dma((8,)),
                dma((segments, 2)), dma((segments, 2)),
            ],
            compiler_params=pltpu.CompilerParams(collective_id=0, has_side_effects=True),
            name="overland",
        )(depth, rainfall, conveyance, flow_dir, outlet))

    placed = P("row", "col")
    return jax.shard_map(
        on_device, mesh=mesh, in_specs=(placed,) * 5, out_specs=(placed, placed), check_vma=False)
```

```python
import functools

import jax
import jax.numpy as jnp
from jax import lax
from jax.experimental import pallas as pl
from jax.experimental.pallas import tpu as pltpu
from jax.sharding import PartitionSpec as P

SUBSTEPS = 3
PASSES = 64
MARGIN = 32
INNER = 16
LANES = 128
NEAR = 4
MESH = pl.DeviceIdType.MESH
OFFSETS = ((0, 1), (1, 1), (1, 0), (1, -1), (0, -1), (-1, -1), (-1, 0), (-1, 1))
SIDES = ((-1, 0), (1, 0), (0, -1), (0, 1), (-1, -1), (-1, 1), (1, -1), (1, 1))
VERTICAL = ((-1, 0), (1, 0))


def starts(first, last):
    made = list(range(first, last - 7, 8))
    if made[-1] + 8 < last:
        made.append(last - 8)
    return made


def kernel(
    rows, cols, nrow, ncol,
    depth, rainfall, conveyance, flow_dir, outlet, new_depth, discharge,
    near, flow, out_of, pack, landed, route, level, sent, rest, masks, state, far, final,
    in_sem, out_sem, near_ssem, near_rsem, route_ssem, route_rsem, far_ssem, far_rsem,
):
    strips = cols // LANES
    mid, left, right = strips, strips + 1, strips + 2
    inner_order = list(range(strips)) + [mid]
    near_order = [left] + list(range(strips)) + [right]
    top = MARGIN + 8
    end = top + rows
    base = 16
    me_r, me_c = lax.axis_index("row"), lax.axis_index("col")
    lane = lax.broadcasted_iota(jnp.int32, (8, LANES), 1)
    zero = jnp.zeros((8, LANES), jnp.float32)
    own = pl.ds(base, rows)

    def present(dr, dc):
        r, c = me_r + dr, me_c + dc
        return (r >= 0) & (r < nrow) & (c >= 0) & (c < ncol)

    loads = []
    for a, (source, target) in enumerate((
        (flow_dir, flow), (outlet, out_of), (depth, near.at[0]), (rainfall, near.at[1]), (conveyance, near.at[2]),
    )):
        for w in range(strips):
            loads.append(pltpu.make_async_copy(
                source.at[:, pl.ds(w * LANES, LANES)],
                target.at[w, pl.ds(0, rows) if a < 2 else own, :], in_sem.at[a, w]))
    for load in loads:
        load.start()

    def clear(ref, first, last):
        for r in range(first, last, 8):
            ref[pl.ds(r, 8), :] = zero

    for half in range(2):
        for w in near_order:
            clear(landed.at[half, w], 8, 8 + 4 * NEAR)
        for seg in range(PASSES // MARGIN):
            for w in inner_order:
                clear(far.at[seg, half, w], 0, MARGIN)
    for a in range(4):
        for w in (left, right):
            clear(near.at[a, w], base, base + rows)
    for w in inner_order:
        clear(route.at[w], top - MARGIN, top)
        clear(route.at[w], end, end + MARGIN)

    barrier = pltpu.get_barrier_semaphore()
    neighbours = jnp.int32(0)
    for dr, dc in SIDES:
        here = present(dr, dc)
        neighbours = neighbours + here.astype(jnp.int32)

        @pl.when(here)
        def _():
            pl.semaphore_signal(barrier, inc=1, device_id=(me_r + dr, me_c + dc), device_id_type=MESH)

    def remote(side, src, dst, ssem, rsem):
        return side, pltpu.make_async_remote_copy(
            src_ref=src, dst_ref=dst, send_sem=ssem, recv_sem=rsem,
            device_id=(me_r + side[0], me_c + side[1]), device_id_type=MESH)

    def start_all(made):
        for (dr, dc), copy in made:
            pl.when(present(dr, dc))(lambda: copy.start())

    def arrive_all(made):
        for (dr, dc), copy in made:
            pl.when(present(-dr, -dc))(lambda: copy.wait_recv())

    def leave_all(made):
        for (dr, dc), copy in made:
            pl.when(present(dr, dc))(lambda: copy.wait_send())

    near_copies = []
    for d, (dr, dc) in enumerate(SIDES):
        if dr == 0:
            src = near.at[:, 0 if dc < 0 else strips - 1, own, :]
            dst = near.at[:, right if dc < 0 else left, own, :]
        else:
            half, at = (0 if dr < 0 else 1), pl.ds(8, 4 * NEAR)
            if dc == 0:
                src, dst = pack.at[half, :, at, :], landed.at[1 - half, pl.ds(0, strips), at, :]
            else:
                src = pack.at[half, 0 if dc < 0 else strips - 1, at, :]
                dst = landed.at[1 - half, right if dc < 0 else left, at, :]
        near_copies.append(remote((dr, dc), src, dst, near_ssem.at[d], near_rsem.at[d]))

    edge = {-1: (pl.ds(top, MARGIN), pl.ds(end, MARGIN)), 1: (pl.ds(end - MARGIN, MARGIN), pl.ds(top - MARGIN, MARGIN))}
    route_copies, route_mid_copies = [], []
    for d, (dr, dc) in enumerate(VERTICAL):
        source, target = edge[dr]
        route_copies.append(remote(
            (dr, dc), route.at[pl.ds(0, strips), source, :], route.at[pl.ds(0, strips), target, :],
            route_ssem.at[0, d], route_rsem.at[0, d]))
        route_mid_copies.append(remote(
            (dr, dc), route.at[mid, source, :], route.at[mid, target, :], route_ssem.at[1, d], route_rsem.at[1, d]))

    def far_copies(source, seg):
        return [
            remote((dr, dc), source.at[:, edge[dr][0], :], far.at[seg, 1 - d], far_ssem.at[seg, d], far_rsem.at[seg, d])
            for d, (dr, dc) in enumerate(VERTICAL)
        ]

    for load in loads:
        load.wait()
    for w in range(strips):
        for r in range(0, rows, 8):
            at, here = pl.ds(r, 8), pl.ds(base + r, 8)
            code = flow[w, at, :]
            kind = jnp.where(out_of[w, at, :] == 1, 0, code + 1).astype(jnp.float32)
            near[3, w, here, :] = kind
            route[w, pl.ds(top + r, 8), :] = kind
            length = jnp.where(code % 2 == 1, jnp.float32(0.70710678), jnp.float32(1.0))
            near[2, w, here, :] = near[2, w, here, :] * length
        for a in range(4):
            pack[0, w, pl.ds(8 + NEAR * a, 8), :] = near[a, w, pl.ds(base, 8), :]
        for a in reversed(range(4)):
            pack[1, w, pl.ds(8 + NEAR * (a - 1), 8), :] = near[a, w, pl.ds(base + rows - 8, 8), :]

    pl.semaphore_wait(barrier, neighbours)
    start_all(near_copies)
    start_all(route_copies)

    arrive_all(near_copies)
    for r in range(0, rows, 8):
        here = pl.ds(base + r, 8)
        route[mid, pl.ds(top + r, 8), :] = jnp.where(lane < LANES // 2, near[3, right, here, :], near[3, left, here, :])
    start_all(route_mid_copies)
    for w in near_order:
        for a in range(4):
            near[a, w, pl.ds(base - 8, 8), :] = landed[0, w, pl.ds(8 + NEAR * (a - 1), 8), :]
            near[a, w, pl.ds(base + rows, 8), :] = landed[1, w, pl.ds(8 + NEAR * a, 8), :]

    def make_masks(codes, shift, w, r):
        around = {di: codes[w, pl.ds(r + shift - di, 8), :] for di in (-1, 0, 1)}
        for k, (di, dj) in enumerate(OFFSETS):
            masks[k, w, pl.ds(r, 8), :] = jnp.where(
                around[di] == jnp.float32(k + 1), jnp.float32(1.0), jnp.float32(0.0))

    def inflow(source, shift, order, held, r):
        east, west, still = [], [], []
        count = len(order)
        for w in order:
            x = {di: source[w, pl.ds(r + shift - di, 8), :] for di in (-1, 0, 1)}
            term = [masks[k, w, pl.ds(r, 8), :] * x[di] for k, (di, _) in enumerate(OFFSETS)]
            east.append(term[0] + term[1] + term[7])
            west.append(term[3] + term[4] + term[5])
            still.append(held[w, pl.ds(r + shift, 8), :] + term[2] + term[6])
        east = [pltpu.roll(x, 1, 1) for x in east]
        west = [pltpu.roll(x, LANES - 1, 1) for x in west]
        return [
            still[i]
            + jnp.where(lane == 0, east[i - 1], east[i])
            + jnp.where(lane == LANES - 1, west[(i + 1) % count], west[i])
            for i in range(count)
        ]

    for w in near_order:
        for r in starts(top - NEAR, end + NEAR):
            make_masks(near.at[3], base - top, w, r)
    for r in starts(top + 1, end - 1):
        make_masks(route, 0, mid, r)
    for step in range(SUBSTEPS):
        held = near.at[0] if step == 0 else final
        for w in near_order:
            for r in starts(base - NEAR, base + rows + NEAR):
                at = pl.ds(r, 8)
                h = held[w, at, :]
                factor = near[2, w, at, :] * jnp.exp(jnp.log(h) * jnp.float32(2.0 / 3.0))
                out = h * (factor / (1.0 + factor))
                sent[w, at, :] = out
                rest[w, at, :] = h + near[1, w, at, :] - out
        if step < SUBSTEPS - 1:
            for r in starts(top - NEAR, end + NEAR):
                new = inflow(sent, base - top, near_order, rest, r)
                for w, value in zip(near_order, new):
                    final[w, pl.ds(r + base - top, 8), :] = value
    for r in range(top, end, 8):
        new = inflow(sent, base - top, near_order, rest, r)
        for w, value in enumerate(new[1:-1] + [jnp.where(lane < LANES // 2, new[-1], new[0])]):
            level[w, pl.ds(r, 8), :] = value
            state[0, w, pl.ds(r, 8), :] = value

    start_all(far_copies(level, 0))
    stores = [
        pltpu.make_async_copy(
            level.at[w, pl.ds(top, rows), :], new_depth.at[:, pl.ds(w * LANES, LANES)], out_sem.at[0, w])
        for w in range(strips)
    ]
    for store in stores:
        store.start()

    lanes = lax.broadcasted_iota(jnp.int32, (strips + 1, 8, LANES), 2)

    def one_pass(p, blocks):
        for r in blocks:
            x = {di: state[p, :, pl.ds(r - di, 8), :] for di in (-1, 0, 1)}
            term = [masks[k, pl.ds(0, strips + 1), pl.ds(r, 8), :] * x[di] for k, (di, _) in enumerate(OFFSETS)]
            east = pltpu.roll(term[0] + term[1] + term[7], 1, 2)
            west = pltpu.roll(term[3] + term[4] + term[5], LANES - 1, 2)
            still = level[:, pl.ds(r, 8), :] + term[2] + term[6]
            before = jnp.concatenate([east[strips:], east[:strips]], axis=0)
            after = jnp.concatenate([west[1:], west[:1]], axis=0)
            value = still + jnp.where(lanes == 0, before, east) + jnp.where(lanes == LANES - 1, after, west)
            state[p + 1, :, pl.ds(r, 8), :] = value
            if p == MARGIN - 1:
                state[0, :, pl.ds(r, 8), :] = value

    def segment(seg, carry):
        for p in range(INNER):
            one_pass(p, starts(top + p + 1, end - p - 1))

        @pl.when(seg == 0)
        def _():
            arrive_all(route_copies)
            arrive_all(route_mid_copies)
            for w in inner_order:
                for r in range(top - MARGIN, top + (8 if w == mid else 0), 8):
                    make_masks(route, 0, w, r)
                for r in range(end - (8 if w == mid else 0), end + MARGIN, 8):
                    make_masks(route, 0, w, r)

        arrive_all(far_copies(level, seg))
        leave_all(far_copies(level, seg))
        for w in inner_order:
            for r in range(0, MARGIN, 8):
                state[0, w, pl.ds(top - MARGIN + r, 8), :] = far[seg, 0, w, pl.ds(r, 8), :]
                state[0, w, pl.ds(end + r, 8), :] = far[seg, 1, w, pl.ds(r, 8), :]

        @pl.when(seg == 0)
        def _():
            for w in inner_order:
                for r in range(0, MARGIN, 8):
                    level[w, pl.ds(top - MARGIN + r, 8), :] = far[0, 0, w, pl.ds(r, 8), :]
                    level[w, pl.ds(end + r, 8), :] = far[0, 1, w, pl.ds(r, 8), :]

        for p in range(MARGIN):
            above, below = top - MARGIN + p + 1, end + MARGIN - p - 1
            if p < INNER:
                one_pass(p, starts(above, above + MARGIN) + starts(below - MARGIN, below))
            else:
                one_pass(p, starts(above, below))

        @pl.when(seg == 0)
        def _():
            start_all(far_copies(state.at[MARGIN], 1))

        return carry

    lax.fori_loop(0, PASSES // MARGIN, segment, 0)

    for w in range(strips):
        for r in range(0, rows, 8):
            final[w, pl.ds(base + r, 8), :] = jnp.log(1.0 + state[MARGIN, w, pl.ds(top + r, 8), :])
    ends = [
        pltpu.make_async_copy(
            final.at[w, own, :], discharge.at[:, pl.ds(w * LANES, LANES)], out_sem.at[1, w])
        for w in range(strips)
    ]
    for store in ends:
        store.start()
    leave_all(near_copies)
    leave_all(route_copies)
    leave_all(route_mid_copies)
    for store in stores + ends:
        store.wait()


def solution(mesh):
    nrow, ncol = mesh.shape["row"], mesh.shape["col"]

    def on_device(depth, rainfall, conveyance, flow_dir, outlet):
        rows, cols = depth.shape
        strips = cols // LANES
        high = rows + 2 * MARGIN + 16
        low = rows + 32
        f32 = functools.partial(pltpu.VMEM, dtype=jnp.float32)
        dma = pltpu.SemaphoreType.DMA
        segments = PASSES // MARGIN
        return tuple(pl.pallas_call(
            functools.partial(kernel, rows, cols, nrow, ncol),
            out_shape=[jax.ShapeDtypeStruct((rows, cols), jnp.float32)] * 2,
            in_specs=[pl.BlockSpec(memory_space=pl.ANY)] * 5,
            out_specs=[pl.BlockSpec(memory_space=pl.ANY)] * 2,
            scratch_shapes=[
                f32((4, strips + 3, low, LANES)),
                pltpu.VMEM((strips, rows, LANES), jnp.int32),
                pltpu.VMEM((strips, rows, LANES), jnp.int32),
                f32((2, strips, 32, LANES)),
                f32((2, strips + 3, 32, LANES)),
                f32((strips + 1, high, LANES)),
                f32((strips + 1, high, LANES)),
                f32((strips + 3, low, LANES)),
                f32((strips + 3, low, LANES)),
                f32((8, strips + 3, high, LANES)),
                f32((MARGIN + 1, strips + 1, high, LANES)),
                f32((segments, 2, strips + 1, MARGIN, LANES)),
                f32((strips + 3, low, LANES)),
                dma((5, strips)),
                dma((2, strips)),
                dma((8,)), dma((8,)), dma((2, 2)), dma((2, 2)),
                dma((segments, 2)), dma((segments, 2)),
            ],
            compiler_params=pltpu.CompilerParams(collective_id=0, has_side_effects=True),
            name="overland",
        )(depth, rainfall, conveyance, flow_dir, outlet))

    placed = P("row", "col")
    return jax.shard_map(
        on_device, mesh=mesh, in_specs=(placed,) * 5, out_specs=(placed, placed), check_vma=False)
```

```python
import functools

import jax
import jax.numpy as jnp
from jax import lax
from jax.experimental import pallas as pl
from jax.experimental.pallas import tpu as pltpu
from jax.sharding import PartitionSpec as P

SUBSTEPS = 3
PASSES = 64
MARGIN = 32
INNER = 24
LANES = 128
NEAR = 4
MESH = pl.DeviceIdType.MESH
OFFSETS = ((0, 1), (1, 1), (1, 0), (1, -1), (0, -1), (-1, -1), (-1, 0), (-1, 1))
SIDES = ((-1, 0), (1, 0), (0, -1), (0, 1), (-1, -1), (-1, 1), (1, -1), (1, 1))
VERTICAL = ((-1, 0), (1, 0))


def starts(first, last):
    made = list(range(first, last - 7, 8))
    if made[-1] + 8 < last:
        made.append(last - 8)
    return made


def to_ring(values):
    count = len(values)
    lane = lax.broadcasted_iota(jnp.int32, values[0].shape, 1)
    made = []
    for w in range(count):
        n = count * lane + w
        at = n & (LANES - 1)
        out = jnp.take_along_axis(values[0], at, axis=1)
        for k in range(1, count):
            out = jnp.where(n >= k * LANES, jnp.take_along_axis(values[k], at, axis=1), out)
        made.append(out)
    return made


def from_ring(values, strip):
    count = len(values)
    n = lax.broadcasted_iota(jnp.int32, values[0].shape, 1) + strip * LANES
    at = (n * ((1 << 18) // count + 1)) >> 18
    which = n - count * at
    out = jnp.take_along_axis(values[0], at, axis=1)
    for k in range(1, count):
        out = jnp.where(which == k, jnp.take_along_axis(values[k], at, axis=1), out)
    return out


def kernel(
    rows, cols, nrow, ncol,
    depth, rainfall, conveyance, flow_dir, outlet, new_depth, runoff,
    near, flow, out_of, pack, landed, route, ring_route, level, sent, rest, near_masks, masks, state, far, final,
    in_sem, near_ssem, near_rsem, route_ssem, route_rsem, far_ssem, far_rsem,
):
    strips = cols // LANES
    mid, left, right = strips, strips + 1, strips + 2
    inner_order = list(range(strips)) + [mid]
    near_order = [left] + list(range(strips)) + [right]
    top = MARGIN + 8
    end = top + rows
    base = 16
    me_r, me_c = lax.axis_index("row"), lax.axis_index("col")
    lane = lax.broadcasted_iota(jnp.int32, (8, LANES), 1)
    zero = jnp.zeros((8, LANES), jnp.float32)
    own = pl.ds(base, rows)

    def present(dr, dc):
        r, c = me_r + dr, me_c + dc
        return (r >= 0) & (r < nrow) & (c >= 0) & (c < ncol)

    loads = []
    for a, (source, target) in enumerate((
        (flow_dir, flow), (outlet, out_of), (depth, near.at[0]), (rainfall, near.at[1]), (conveyance, near.at[2]),
    )):
        for w in range(strips):
            loads.append(pltpu.make_async_copy(
                source.at[:, pl.ds(w * LANES, LANES)],
                target.at[w, pl.ds(0, rows) if a < 2 else own, :], in_sem.at[a, w]))
    for load in loads:
        load.start()

    def clear(ref, first, last):
        for r in range(first, last, 8):
            ref[pl.ds(r, 8), :] = zero

    for half in range(2):
        for w in near_order:
            clear(landed.at[half, w], 8, 8 + 4 * NEAR)
        for seg in range(PASSES // MARGIN):
            for w in inner_order:
                clear(far.at[seg, half, w], 0, MARGIN)
    for a in range(4):
        for w in (left, right):
            clear(near.at[a, w], base, base + rows)
    for w in inner_order:
        clear(route.at[w], top - MARGIN, top)
        clear(route.at[w], end, end + MARGIN)

    barrier = pltpu.get_barrier_semaphore()
    neighbours = jnp.int32(0)
    for dr, dc in SIDES:
        here = present(dr, dc)
        neighbours = neighbours + here.astype(jnp.int32)

        @pl.when(here)
        def _():
            pl.semaphore_signal(barrier, inc=1, device_id=(me_r + dr, me_c + dc), device_id_type=MESH)

    def remote(side, src, dst, ssem, rsem):
        return side, pltpu.make_async_remote_copy(
            src_ref=src, dst_ref=dst, send_sem=ssem, recv_sem=rsem,
            device_id=(me_r + side[0], me_c + side[1]), device_id_type=MESH)

    def start_all(made):
        for (dr, dc), copy in made:
            pl.when(present(dr, dc))(lambda: copy.start())

    def arrive_all(made):
        for (dr, dc), copy in made:
            pl.when(present(-dr, -dc))(lambda: copy.wait_recv())

    def leave_all(made):
        for (dr, dc), copy in made:
            pl.when(present(dr, dc))(lambda: copy.wait_send())

    near_copies = []
    for d, (dr, dc) in enumerate(SIDES):
        if dr == 0:
            src = near.at[:, 0 if dc < 0 else strips - 1, own, :]
            dst = near.at[:, right if dc < 0 else left, own, :]
        else:
            half, at = (0 if dr < 0 else 1), pl.ds(8, 4 * NEAR)
            if dc == 0:
                src, dst = pack.at[half, :, at, :], landed.at[1 - half, pl.ds(0, strips), at, :]
            else:
                src = pack.at[half, 0 if dc < 0 else strips - 1, at, :]
                dst = landed.at[1 - half, right if dc < 0 else left, at, :]
        near_copies.append(remote((dr, dc), src, dst, near_ssem.at[d], near_rsem.at[d]))

    edge = {-1: (pl.ds(top, MARGIN), pl.ds(end, MARGIN)), 1: (pl.ds(end - MARGIN, MARGIN), pl.ds(top - MARGIN, MARGIN))}
    route_copies, route_mid_copies = [], []
    for d, (dr, dc) in enumerate(VERTICAL):
        source, target = edge[dr]
        route_copies.append(remote(
            (dr, dc), route.at[pl.ds(0, strips), source, :], route.at[pl.ds(0, strips), target, :],
            route_ssem.at[0, d], route_rsem.at[0, d]))
        route_mid_copies.append(remote(
            (dr, dc), route.at[mid, source, :], route.at[mid, target, :], route_ssem.at[1, d], route_rsem.at[1, d]))

    def far_copies(source, seg):
        return [
            remote((dr, dc), source.at[:, edge[dr][0], :], far.at[seg, 1 - d], far_ssem.at[seg, d], far_rsem.at[seg, d])
            for d, (dr, dc) in enumerate(VERTICAL)
        ]

    for load in loads:
        load.wait()
    for w in range(strips):
        for r in range(0, rows, 8):
            at, here = pl.ds(r, 8), pl.ds(base + r, 8)
            code = flow[w, at, :]
            kind = jnp.where(out_of[w, at, :] == 1, 0, code + 1).astype(jnp.float32)
            near[3, w, here, :] = kind
            route[w, pl.ds(top + r, 8), :] = kind
            length = jnp.where(code % 2 == 1, jnp.float32(0.70710678), jnp.float32(1.0))
            near[2, w, here, :] = near[2, w, here, :] * length
        for a in range(4):
            pack[0, w, pl.ds(8 + NEAR * a, 8), :] = near[a, w, pl.ds(base, 8), :]
        for a in reversed(range(4)):
            pack[1, w, pl.ds(8 + NEAR * (a - 1), 8), :] = near[a, w, pl.ds(base + rows - 8, 8), :]

    pl.semaphore_wait(barrier, neighbours)
    start_all(near_copies)
    start_all(route_copies)

    def make_masks(target, codes, w, r):
        around = {di: codes[w, pl.ds(r - di, 8), :] for di in (-1, 0, 1)}
        for k, (di, dj) in enumerate(OFFSETS):
            target[k, w, pl.ds(r, 8), :] = jnp.where(
                around[di] == jnp.float32(k + 1), jnp.float32(1.0), jnp.float32(0.0))

    def inflow(r):
        east, west, still = [], [], []
        here = pl.ds(r, 8)
        count = len(near_order)
        for w in near_order:
            x = {di: sent[w, pl.ds(r - di, 8), :] for di in (-1, 0, 1)}
            term = [near_masks[k, w, here, :] * x[di] for k, (di, _) in enumerate(OFFSETS)]
            east.append(term[0] + term[1] + term[7])
            west.append(term[3] + term[4] + term[5])
            still.append(rest[w, here, :] + term[2] + term[6])
        east = [pltpu.roll(x, 1, 1) for x in east]
        west = [pltpu.roll(x, LANES - 1, 1) for x in west]
        return [
            still[i]
            + jnp.where(lane == 0, east[i - 1], east[i])
            + jnp.where(lane == LANES - 1, west[(i + 1) % count], west[i])
            for i in range(count)
        ]

    def outflow(held, w, r):
        at = pl.ds(r, 8)
        h = held[w, at, :]
        factor = near[2, w, at, :] * jnp.exp(jnp.log(h) * jnp.float32(2.0 / 3.0))
        out = h * (factor / (1.0 + factor))
        sent[w, at, :] = out
        rest[w, at, :] = h + near[1, w, at, :] - out

    for w in range(strips):
        for r in starts(base + 1, base + rows - 1):
            make_masks(near_masks, near.at[3], w, r)
        for r in range(base, base + rows, 8):
            outflow(near.at[0], w, r)

    arrive_all(near_copies)
    for r in range(0, rows, 8):
        here = pl.ds(base + r, 8)
        route[mid, pl.ds(top + r, 8), :] = jnp.where(lane < LANES // 2, near[3, right, here, :], near[3, left, here, :])
    start_all(route_mid_copies)
    for w in near_order:
        for a in range(4):
            near[a, w, pl.ds(base - 8, 8), :] = landed[0, w, pl.ds(8 + NEAR * (a - 1), 8), :]
            near[a, w, pl.ds(base + rows, 8), :] = landed[1, w, pl.ds(8 + NEAR * a, 8), :]

    reach = starts(base - NEAR, base + rows + NEAR)
    for w in near_order:
        for r in reach if w >= strips else (base - 7, base + rows - 1):
            make_masks(near_masks, near.at[3], w, r)
    for step in range(SUBSTEPS):
        for w in near_order:
            for r in (base - 8, base + rows) if step == 0 and w < strips else reach:
                outflow(near.at[0] if step == 0 else final, w, r)
        if step < SUBSTEPS - 1:
            for r in reach:
                for w, value in zip(near_order, inflow(r)):
                    final[w, pl.ds(r, 8), :] = value
    for r in range(0, rows, 8):
        new = inflow(base + r)
        for w in range(strips):
            new_depth[pl.ds(r, 8), pl.ds(w * LANES, LANES)] = new[1 + w]
        ring = to_ring(new[1:-1] + [jnp.where(lane < LANES // 2, new[-1], new[0])])
        for w, value in enumerate(ring):
            level[w, pl.ds(top + r, 8), :] = value
            state[0, w, pl.ds(top + r, 8), :] = value

    start_all(far_copies(level, 0))

    def ring_routes(first, last):
        for r in range(first, last, 8):
            for w, value in enumerate(to_ring([route[w, pl.ds(r, 8), :] for w in inner_order])):
                ring_route[w, pl.ds(r, 8), :] = value

    ring_routes(top, end)
    for w in inner_order:
        for r in starts(top + 1, end - 1):
            make_masks(masks, ring_route, w, r)

    def one_pass(p, blocks):
        for r in blocks:
            here = pl.ds(r, 8)
            x = {di: state[p, :, pl.ds(r - di, 8), :] for di in (-1, 0, 1)}
            term = [masks[k, :, here, :] * x[di] for k, (di, _) in enumerate(OFFSETS)]
            east = term[0] + term[1] + term[7]
            west = term[3] + term[4] + term[5]
            still = level[:, here, :] + term[2] + term[6]
            east = jnp.concatenate([pltpu.roll(east[strips:], 1, 2), east[:strips]], axis=0)
            west = jnp.concatenate([west[1:], pltpu.roll(west[:1], LANES - 1, 2)], axis=0)
            value = still + east + west
            state[p + 1, :, here, :] = value
            if p == MARGIN - 1:
                state[0, :, here, :] = value

    def halo(seg, half):
        first = end if half else top - MARGIN
        for w in inner_order:
            for r in range(0, MARGIN, 8):
                state[0, w, pl.ds(first + r, 8), :] = far[seg, half, w, pl.ds(r, 8), :]

        @pl.when(seg == 0)
        def _():
            for w in inner_order:
                for r in range(0, MARGIN, 8):
                    level[w, pl.ds(first + r, 8), :] = far[0, half, w, pl.ds(r, 8), :]

    def segment(seg, carry):
        for p in range(INNER):
            one_pass(p, starts(top + p + 1, end - p - 1))

        @pl.when(seg == 0)
        def _():
            arrive_all(route_copies)
            arrive_all(route_mid_copies)
            ring_routes(top - MARGIN, top)
            ring_routes(end, end + MARGIN)
            for w in inner_order:
                for r in (*range(top - MARGIN, top + 8, 8), *range(end - 8, end + MARGIN, 8)):
                    make_masks(masks, ring_route, w, r)

        arrive_all(far_copies(level, seg))
        leave_all(far_copies(level, seg))
        halo(seg, 0)
        halo(seg, 1)
        for p in range(MARGIN):
            above, below = top - MARGIN + p + 1, end + MARGIN - p - 1
            if p < INNER:
                one_pass(p, starts(above, above + MARGIN) + starts(below - MARGIN, below))
            else:
                one_pass(p, starts(above, below))

        @pl.when(seg == 0)
        def _():
            start_all(far_copies(state.at[MARGIN], 1))

        return carry

    lax.fori_loop(0, PASSES // MARGIN, segment, 0)

    for w in inner_order:
        for r in range(0, rows, 8):
            runoff[w, pl.ds(r, 8), :] = state[MARGIN, w, pl.ds(top + r, 8), :]
    leave_all(near_copies)
    leave_all(route_copies)
    leave_all(route_mid_copies)


def finish(level, runoff, new_depth, discharge, logs, sems):
    first = pltpu.make_async_copy(level, new_depth, sems.at[0])
    first.start()
    rows, cols = level.shape
    for r in range(0, rows, 8):
        ring = [jnp.log(1.0 + runoff[w, pl.ds(r, 8), :]) for w in range(runoff.shape[0])]
        for w in range(cols // LANES):
            logs[pl.ds(r, 8), pl.ds(w * LANES, LANES)] = from_ring(ring, w)
    second = pltpu.make_async_copy(logs, discharge, sems.at[1])
    second.start()
    first.wait()
    second.wait()


def solution(mesh):
    nrow, ncol = mesh.shape["row"], mesh.shape["col"]

    def on_device(depth, rainfall, conveyance, flow_dir, outlet):
        rows, cols = depth.shape
        strips = cols // LANES
        high = rows + 2 * MARGIN + 16
        low = rows + 32
        f32 = functools.partial(pltpu.VMEM, dtype=jnp.float32)
        dma = pltpu.SemaphoreType.DMA
        segments = PASSES // MARGIN
        pin = lambda x: pltpu.with_memory_space_constraint(x, pltpu.HBM)
        depth, rainfall, conveyance, flow_dir, outlet = map(pin, (depth, rainfall, conveyance, flow_dir, outlet))
        level, runoff = pl.pallas_call(
            functools.partial(kernel, rows, cols, nrow, ncol),
            out_shape=[
                jax.ShapeDtypeStruct((rows, cols), jnp.float32),
                jax.ShapeDtypeStruct((strips + 1, rows, LANES), jnp.float32),
            ],
            in_specs=[pl.BlockSpec(memory_space=pl.ANY)] * 5,
            out_specs=[pl.BlockSpec(memory_space=pltpu.VMEM)] * 2,
            scratch_shapes=[
                f32((4, strips + 3, low, LANES)),
                pltpu.VMEM((strips, rows, LANES), jnp.int32),
                pltpu.VMEM((strips, rows, LANES), jnp.int32),
                f32((2, strips, 32, LANES)),
                f32((2, strips + 3, 32, LANES)),
                f32((strips + 1, high, LANES)),
                f32((strips + 1, high, LANES)),
                f32((strips + 1, high, LANES)),
                f32((strips + 3, low, LANES)),
                f32((strips + 3, low, LANES)),
                f32((8, strips + 3, low, LANES)),
                f32((8, strips + 1, high, LANES)),
                f32((MARGIN + 1, strips + 1, high, LANES)),
                f32((segments, 2, strips + 1, MARGIN, LANES)),
                f32((strips + 3, low, LANES)),
                dma((5, strips)),
                dma((8,)), dma((8,)), dma((2, 2)), dma((2, 2)),
                dma((segments, 2)), dma((segments, 2)),
            ],
            compiler_params=pltpu.CompilerParams(
                collective_id=0, has_side_effects=True, vmem_limit_bytes=32 * 2**20),
            name="overland",
        )(depth, rainfall, conveyance, flow_dir, outlet)
        return tuple(pl.pallas_call(
            finish,
            out_shape=[jax.ShapeDtypeStruct((rows, cols), jnp.float32)] * 2,
            in_specs=[pl.BlockSpec(memory_space=pltpu.VMEM)] * 2,
            out_specs=[pl.BlockSpec(memory_space=pl.ANY)] * 2,
            scratch_shapes=[f32((rows, cols)), dma((2,))],
            compiler_params=pltpu.CompilerParams(vmem_limit_bytes=4 * 2**20),
            name="finish",
        )(level, runoff))

    placed = P("row", "col")
    return jax.shard_map(
        on_device, mesh=mesh, in_specs=(placed,) * 5, out_specs=(placed, placed), check_vma=False)
```

```python
import functools

import jax
import jax.numpy as jnp
from jax import lax
from jax.experimental import pallas as pl
from jax.experimental.pallas import tpu as pltpu
from jax.sharding import PartitionSpec as P

SUBSTEPS = 3
PASSES = 64
MARGIN = 32
LANES = 128
NEAR = 4
MESH = pl.DeviceIdType.MESH
OFFSETS = ((0, 1), (1, 1), (1, 0), (1, -1), (0, -1), (-1, -1), (-1, 0), (-1, 1))
SIDES = ((-1, 0), (1, 0), (0, -1), (0, 1), (-1, -1), (-1, 1), (1, -1), (1, 1))
VERTICAL = ((-1, 0), (1, 0))


def starts(first, last):
    made = list(range(first, last - 7, 8))
    if made[-1] + 8 < last:
        made.append(last - 8)
    return made


def to_ring(values):
    count = len(values)
    lane = lax.broadcasted_iota(jnp.int32, values[0].shape, 1)
    made = []
    for w in range(count):
        n = count * lane + w
        at = n & (LANES - 1)
        out = jnp.take_along_axis(values[0], at, axis=1)
        for k in range(1, count):
            out = jnp.where(n >= k * LANES, jnp.take_along_axis(values[k], at, axis=1), out)
        made.append(out)
    return made


def from_ring(values, strip):
    count = len(values)
    n = lax.broadcasted_iota(jnp.int32, values[0].shape, 1) + strip * LANES
    at = (n * ((1 << 18) // count + 1)) >> 18
    which = n - count * at
    out = jnp.take_along_axis(values[0], at, axis=1)
    for k in range(1, count):
        out = jnp.where(which == k, jnp.take_along_axis(values[k], at, axis=1), out)
    return out


def kernel(
    rows, cols, nrow, ncol,
    depth, rainfall, conveyance, flow_dir, outlet, new_depth, runoff,
    near, flow, out_of, pack, landed, route, ring_route, level, sent, rest, near_masks, masks, state, far, final,
    in_sem, near_ssem, near_rsem, route_ssem, route_rsem, far_ssem, far_rsem,
):
    strips = cols // LANES
    mid, left, right = strips, strips + 1, strips + 2
    inner_order = list(range(strips)) + [mid]
    near_order = [left] + list(range(strips)) + [right]
    top = MARGIN + 8
    end = top + rows
    base = 16
    me_r, me_c = lax.axis_index("row"), lax.axis_index("col")
    lane = lax.broadcasted_iota(jnp.int32, (8, LANES), 1)
    zero = jnp.zeros((8, LANES), jnp.float32)
    own = pl.ds(base, rows)

    def present(dr, dc):
        r, c = me_r + dr, me_c + dc
        return (r >= 0) & (r < nrow) & (c >= 0) & (c < ncol)

    loads = []
    for a, (source, target) in enumerate((
        (flow_dir, flow), (outlet, out_of), (depth, near.at[0]), (rainfall, near.at[1]), (conveyance, near.at[2]),
    )):
        for w in range(strips):
            loads.append(pltpu.make_async_copy(
                source.at[:, pl.ds(w * LANES, LANES)],
                target.at[w, pl.ds(0, rows) if a < 2 else own, :], in_sem.at[a, w]))
    for load in loads:
        load.start()

    def clear(ref, first, last):
        for r in range(first, last, 8):
            ref[pl.ds(r, 8), :] = zero

    for half in range(2):
        for w in near_order:
            clear(landed.at[half, w], 8, 8 + 4 * NEAR)
        for seg in range(PASSES // MARGIN):
            for w in inner_order:
                clear(far.at[seg, half, w], 0, MARGIN)
    for a in range(4):
        for w in (left, right):
            clear(near.at[a, w], base, base + rows)
    for w in inner_order:
        clear(route.at[w], top - MARGIN, top)
        clear(route.at[w], end, end + MARGIN)

    barrier = pltpu.get_barrier_semaphore()
    neighbours = jnp.int32(0)
    for dr, dc in SIDES:
        here = present(dr, dc)
        neighbours = neighbours + here.astype(jnp.int32)

        @pl.when(here)
        def _():
            pl.semaphore_signal(barrier, inc=1, device_id=(me_r + dr, me_c + dc), device_id_type=MESH)

    def remote(side, src, dst, ssem, rsem):
        return side, pltpu.make_async_remote_copy(
            src_ref=src, dst_ref=dst, send_sem=ssem, recv_sem=rsem,
            device_id=(me_r + side[0], me_c + side[1]), device_id_type=MESH)

    def start_all(made):
        for (dr, dc), copy in made:
            pl.when(present(dr, dc))(lambda: copy.start())

    def arrive_all(made):
        for (dr, dc), copy in made:
            pl.when(present(-dr, -dc))(lambda: copy.wait_recv())

    def leave_all(made):
        for (dr, dc), copy in made:
            pl.when(present(dr, dc))(lambda: copy.wait_send())

    near_copies = []
    for d, (dr, dc) in enumerate(SIDES):
        if dr == 0:
            src = near.at[:, 0 if dc < 0 else strips - 1, own, :]
            dst = near.at[:, right if dc < 0 else left, own, :]
        else:
            half, at = (0 if dr < 0 else 1), pl.ds(8, 4 * NEAR)
            if dc == 0:
                src, dst = pack.at[half, :, at, :], landed.at[1 - half, pl.ds(0, strips), at, :]
            else:
                src = pack.at[half, 0 if dc < 0 else strips - 1, at, :]
                dst = landed.at[1 - half, right if dc < 0 else left, at, :]
        near_copies.append(remote((dr, dc), src, dst, near_ssem.at[d], near_rsem.at[d]))

    edge = {-1: (pl.ds(top, MARGIN), pl.ds(end, MARGIN)), 1: (pl.ds(end - MARGIN, MARGIN), pl.ds(top - MARGIN, MARGIN))}
    route_copies, route_mid_copies = [], []
    for d, (dr, dc) in enumerate(VERTICAL):
        source, target = edge[dr]
        route_copies.append(remote(
            (dr, dc), route.at[pl.ds(0, strips), source, :], route.at[pl.ds(0, strips), target, :],
            route_ssem.at[0, d], route_rsem.at[0, d]))
        route_mid_copies.append(remote(
            (dr, dc), route.at[mid, source, :], route.at[mid, target, :], route_ssem.at[1, d], route_rsem.at[1, d]))

    def far_copies(source, seg):
        return [
            remote((dr, dc), source.at[:, edge[dr][0], :], far.at[seg, 1 - d], far_ssem.at[seg, d], far_rsem.at[seg, d])
            for d, (dr, dc) in enumerate(VERTICAL)
        ]

    for load in loads:
        load.wait()
    for w in range(strips):
        for r in range(0, rows, 8):
            at, here = pl.ds(r, 8), pl.ds(base + r, 8)
            code = flow[w, at, :]
            kind = jnp.where(out_of[w, at, :] == 1, 0, code + 1).astype(jnp.float32)
            near[3, w, here, :] = kind
            route[w, pl.ds(top + r, 8), :] = kind
            length = jnp.where(code % 2 == 1, jnp.float32(0.70710678), jnp.float32(1.0))
            near[2, w, here, :] = near[2, w, here, :] * length
        for a in range(4):
            pack[0, w, pl.ds(8 + NEAR * a, 8), :] = near[a, w, pl.ds(base, 8), :]
        for a in reversed(range(4)):
            pack[1, w, pl.ds(8 + NEAR * (a - 1), 8), :] = near[a, w, pl.ds(base + rows - 8, 8), :]

    pl.semaphore_wait(barrier, neighbours)
    start_all(near_copies)
    start_all(route_copies)

    def make_masks(target, codes, w, r):
        around = {di: codes[w, pl.ds(r - di, 8), :] for di in (-1, 0, 1)}
        for k, (di, dj) in enumerate(OFFSETS):
            target[k, w, pl.ds(r, 8), :] = jnp.where(
                around[di] == jnp.float32(k + 1), jnp.float32(1.0), jnp.float32(0.0))

    def inflow(r):
        east, west, still = [], [], []
        here = pl.ds(r, 8)
        count = len(near_order)
        for w in near_order:
            x = {di: sent[w, pl.ds(r - di, 8), :] for di in (-1, 0, 1)}
            term = [near_masks[k, w, here, :] * x[di] for k, (di, _) in enumerate(OFFSETS)]
            east.append(term[0] + term[1] + term[7])
            west.append(term[3] + term[4] + term[5])
            still.append(rest[w, here, :] + term[2] + term[6])
        east = [pltpu.roll(x, 1, 1) for x in east]
        west = [pltpu.roll(x, LANES - 1, 1) for x in west]
        return [
            still[i]
            + jnp.where(lane == 0, east[i - 1], east[i])
            + jnp.where(lane == LANES - 1, west[(i + 1) % count], west[i])
            for i in range(count)
        ]

    def outflow(held, w, r):
        at = pl.ds(r, 8)
        h = held[w, at, :]
        factor = near[2, w, at, :] * jnp.exp(jnp.log(h) * jnp.float32(2.0 / 3.0))
        out = h * (factor / (1.0 + factor))
        sent[w, at, :] = out
        rest[w, at, :] = h + near[1, w, at, :] - out

    for w in range(strips):
        for r in starts(base + 1, base + rows - 1):
            make_masks(near_masks, near.at[3], w, r)
        for r in range(base, base + rows, 8):
            outflow(near.at[0], w, r)

    arrive_all(near_copies)
    for r in range(0, rows, 8):
        here = pl.ds(base + r, 8)
        route[mid, pl.ds(top + r, 8), :] = jnp.where(lane < LANES // 2, near[3, right, here, :], near[3, left, here, :])
    start_all(route_mid_copies)
    for w in near_order:
        for a in range(4):
            near[a, w, pl.ds(base - 8, 8), :] = landed[0, w, pl.ds(8 + NEAR * (a - 1), 8), :]
            near[a, w, pl.ds(base + rows, 8), :] = landed[1, w, pl.ds(8 + NEAR * a, 8), :]

    reach = starts(base - NEAR, base + rows + NEAR)
    for w in near_order:
        for r in reach if w >= strips else (base - 7, base + rows - 1):
            make_masks(near_masks, near.at[3], w, r)
    for step in range(SUBSTEPS):
        for w in near_order:
            for r in (base - 8, base + rows) if step == 0 and w < strips else reach:
                outflow(near.at[0] if step == 0 else final, w, r)
        if step < SUBSTEPS - 1:
            for r in reach:
                for w, value in zip(near_order, inflow(r)):
                    final[w, pl.ds(r, 8), :] = value
    for r in range(0, rows, 8):
        new = inflow(base + r)
        for w in range(strips):
            new_depth[pl.ds(r, 8), pl.ds(w * LANES, LANES)] = new[1 + w]
            final[w, pl.ds(base + r, 8), :] = new[1 + w]
        final[mid, pl.ds(base + r, 8), :] = jnp.where(lane < LANES // 2, new[-1], new[0])

    def level_ring(step, carry):
        for half in range(0, rows // 2, 8):
            r = pl.multiple_of(step * (rows // 2), 8) + half
            for w, value in enumerate(to_ring([final[w, pl.ds(base + r, 8), :] for w in inner_order])):
                level[w, pl.ds(top + r, 8), :] = value
                state[0, w, pl.ds(top + r, 8), :] = value
        return carry

    lax.fori_loop(0, 2, level_ring, 0)
    start_all(far_copies(level, 0))

    def ring_routes(first, last):
        for r in range(first, last, 8):
            for w, value in enumerate(to_ring([route[w, pl.ds(r, 8), :] for w in inner_order])):
                ring_route[w, pl.ds(r, 8), :] = value

    ring_routes(top, end)
    for w in inner_order:
        for r in starts(top + 1, end - 1):
            make_masks(masks, ring_route, w, r)

    def one_pass(p, blocks):
        for r in blocks:
            here = pl.ds(r, 8)
            x = {di: state[p, :, pl.ds(r - di, 8), :] for di in (-1, 0, 1)}
            term = [masks[k, :, here, :] * x[di] for k, (di, _) in enumerate(OFFSETS)]
            east = term[0] + term[1] + term[7]
            west = term[3] + term[4] + term[5]
            still = level[:, here, :] + term[2] + term[6]
            east = jnp.concatenate([pltpu.roll(east[strips:], 1, 2), east[:strips]], axis=0)
            west = jnp.concatenate([west[1:], pltpu.roll(west[:1], LANES - 1, 2)], axis=0)
            value = still + east + west
            state[p + 1, :, here, :] = value
            if p == MARGIN - 1:
                state[0, :, here, :] = value

    def halo(seg, half):
        first = end if half else top - MARGIN
        for w in inner_order:
            for r in range(0, MARGIN, 8):
                state[0, w, pl.ds(first + r, 8), :] = far[seg, half, w, pl.ds(r, 8), :]

        @pl.when(seg == 0)
        def _():
            for w in inner_order:
                for r in range(0, MARGIN, 8):
                    level[w, pl.ds(first + r, 8), :] = far[0, half, w, pl.ds(r, 8), :]

    def top_band(seg):
        arrive_all(far_copies(level, seg)[1:])
        halo(seg, 0)
        for p in range(MARGIN):
            one_pass(p, starts(top - MARGIN + p + 1, top + p + 1)[::-1])

    def bottom_band(seg):
        arrive_all(far_copies(level, seg)[:1])
        halo(seg, 1)
        for p in range(MARGIN):
            one_pass(p, starts(end - p - 1, end + MARGIN - p - 1))

    def segment(seg, carry):
        for p in range(rows // 2 - 1):
            here, stop = top + p + 1, end - p - 1
            one_pass(p, starts(here, stop) if stop - here >= 8 else [here + (stop - here) // 2 - 4])

        @pl.when(seg == 0)
        def _():
            arrive_all(route_copies)
            arrive_all(route_mid_copies)
            ring_routes(top - MARGIN, top)
            ring_routes(end, end + MARGIN)
            for w in inner_order:
                for r in (*range(top - MARGIN, top + 8, 8), *range(end - 8, end + MARGIN, 8)):
                    make_masks(masks, ring_route, w, r)
            top_band(0)
            start_all(far_copies(state.at[MARGIN], 1)[:1])

        leave_all(far_copies(level, seg))
        bottom_band(seg)

        @pl.when(seg == 0)
        def _():
            start_all(far_copies(state.at[MARGIN], 1)[1:])

        @pl.when(seg == 1)
        def _():
            top_band(1)

        return carry

    lax.fori_loop(0, PASSES // MARGIN, segment, 0)

    for w in inner_order:
        for r in range(0, rows, 8):
            runoff[w, pl.ds(r, 8), :] = state[MARGIN, w, pl.ds(top + r, 8), :]
    leave_all(near_copies)
    leave_all(route_copies)
    leave_all(route_mid_copies)


def finish(level, runoff, new_depth, discharge, logs, sems):
    first = pltpu.make_async_copy(level, new_depth, sems.at[0])
    first.start()
    rows, cols = level.shape
    for r in range(0, rows, 8):
        ring = [jnp.log(1.0 + runoff[w, pl.ds(r, 8), :]) for w in range(runoff.shape[0])]
        for w in range(cols // LANES):
            logs[pl.ds(r, 8), pl.ds(w * LANES, LANES)] = from_ring(ring, w)
    second = pltpu.make_async_copy(logs, discharge, sems.at[1])
    second.start()
    first.wait()
    second.wait()


def solution(mesh):
    nrow, ncol = mesh.shape["row"], mesh.shape["col"]

    def on_device(depth, rainfall, conveyance, flow_dir, outlet):
        rows, cols = depth.shape
        strips = cols // LANES
        high = rows + 2 * MARGIN + 16
        low = rows + 32
        f32 = functools.partial(pltpu.VMEM, dtype=jnp.float32)
        dma = pltpu.SemaphoreType.DMA
        segments = PASSES // MARGIN
        pin = lambda x: pltpu.with_memory_space_constraint(x, pltpu.HBM)
        depth, rainfall, conveyance, flow_dir, outlet = map(pin, (depth, rainfall, conveyance, flow_dir, outlet))
        level, runoff = pl.pallas_call(
            functools.partial(kernel, rows, cols, nrow, ncol),
            out_shape=[
                jax.ShapeDtypeStruct((rows, cols), jnp.float32),
                jax.ShapeDtypeStruct((strips + 1, rows, LANES), jnp.float32),
            ],
            in_specs=[pl.BlockSpec(memory_space=pl.ANY)] * 5,
            out_specs=[pl.BlockSpec(memory_space=pltpu.VMEM)] * 2,
            scratch_shapes=[
                f32((4, strips + 3, low, LANES)),
                pltpu.VMEM((strips, rows, LANES), jnp.int32),
                pltpu.VMEM((strips, rows, LANES), jnp.int32),
                f32((2, strips, 32, LANES)),
                f32((2, strips + 3, 32, LANES)),
                f32((strips + 1, high, LANES)),
                f32((strips + 1, high, LANES)),
                f32((strips + 1, high, LANES)),
                f32((strips + 3, low, LANES)),
                f32((strips + 3, low, LANES)),
                f32((8, strips + 3, low, LANES)),
                f32((8, strips + 1, high, LANES)),
                f32((MARGIN + 1, strips + 1, high, LANES)),
                f32((segments, 2, strips + 1, MARGIN, LANES)),
                f32((strips + 3, low, LANES)),
                dma((5, strips)),
                dma((8,)), dma((8,)), dma((2, 2)), dma((2, 2)),
                dma((segments, 2)), dma((segments, 2)),
            ],
            compiler_params=pltpu.CompilerParams(
                collective_id=0, has_side_effects=True, vmem_limit_bytes=32 * 2**20),
            name="overland",
        )(depth, rainfall, conveyance, flow_dir, outlet)
        return tuple(pl.pallas_call(
            finish,
            out_shape=[jax.ShapeDtypeStruct((rows, cols), jnp.float32)] * 2,
            in_specs=[pl.BlockSpec(memory_space=pltpu.VMEM)] * 2,
            out_specs=[pl.BlockSpec(memory_space=pl.ANY)] * 2,
            scratch_shapes=[f32((rows, cols)), dma((2,))],
            compiler_params=pltpu.CompilerParams(vmem_limit_bytes=4 * 2**20),
            name="finish",
        )(level, runoff))

    placed = P("row", "col")
    return jax.shard_map(
        on_device, mesh=mesh, in_specs=(placed,) * 5, out_specs=(placed, placed), check_vma=False)
```

```python
import functools
import math

import jax
import jax.numpy as jnp
from jax import lax
from jax.experimental import pallas as pl
from jax.experimental.pallas import tpu as pltpu
from jax.sharding import PartitionSpec as P

SUBSTEPS = 3
PASSES = 64
MARGIN = 32
LANES = 128
NEAR = 4
MESH = pl.DeviceIdType.MESH
OFFSETS = ((0, 1), (1, 1), (1, 0), (1, -1), (0, -1), (-1, -1), (-1, 0), (-1, 1))
SIDES = ((-1, 0), (1, 0), (0, -1), (0, 1), (-1, -1), (-1, 1), (1, -1), (1, 1))
VERTICAL = ((-1, 0), (1, 0))


def starts(first, last):
    made = list(range(first, last - 7, 8))
    if made[-1] + 8 < last:
        made.append(last - 8)
    return made


def to_ring(values):
    count = len(values)
    lane = lax.broadcasted_iota(jnp.int32, values[0].shape, 1)
    made = []
    for w in range(count):
        n = count * lane + w
        at = n & (LANES - 1)
        out = jnp.take_along_axis(values[0], at, axis=1)
        for k in range(1, count):
            out = jnp.where(n >= k * LANES, jnp.take_along_axis(values[k], at, axis=1), out)
        made.append(out)
    return made


def from_ring(values, strip):
    count = len(values)
    n = lax.broadcasted_iota(jnp.int32, values[0].shape, 1) + strip * LANES
    at = (n * ((1 << 18) // count + 1)) >> 18
    which = n - count * at
    out = jnp.take_along_axis(values[0], at, axis=1)
    for k in range(1, count):
        out = jnp.where(which == k, jnp.take_along_axis(values[k], at, axis=1), out)
    return out


def kernel(
    rows, cols, nrow, ncol,
    depth, rainfall, conveyance, flow_dir, outlet, new_depth, runoff,
    near, plain, flow, out_of, pack, landed, route, ring_route, level, sent, rest, near_masks, masks, state, far, final,
    in_sem, near_ssem, near_rsem, route_ssem, route_rsem, far_ssem, far_rsem,
):
    strips = cols // LANES
    mid, left, right = strips, strips + 1, strips + 2
    inner_order = list(range(strips)) + [mid]
    near_order = [left] + list(range(strips)) + [right]
    top = MARGIN + 8
    end = top + rows
    base = 16
    me_r, me_c = lax.axis_index("row"), lax.axis_index("col")
    lane = lax.broadcasted_iota(jnp.int32, (8, LANES), 1)
    zero = jnp.zeros((8, LANES), jnp.float32)
    own = pl.ds(base, rows)

    def present(dr, dc):
        r, c = me_r + dr, me_c + dc
        return (r >= 0) & (r < nrow) & (c >= 0) & (c < ncol)

    barrier = pltpu.get_barrier_semaphore()
    neighbours = jnp.int32(0)
    for dr, dc in SIDES:
        here = present(dr, dc)
        neighbours = neighbours + here.astype(jnp.int32)

        @pl.when(here)
        def _():
            pl.semaphore_signal(barrier, inc=1, device_id=(me_r + dr, me_c + dc), device_id_type=MESH)

    loads = [
        pltpu.make_async_copy(source, target, in_sem.at[a])
        for a, (source, target) in enumerate((
            (flow_dir, flow), (outlet, out_of), (conveyance, plain.at[2]), (depth, plain.at[0]), (rainfall, plain.at[1]),
        ))
    ]
    for load in loads:
        load.start()

    def clear(ref, first, last):
        for r in range(first, last, 8):
            ref[pl.ds(r, 8), :] = zero

    for half, dr in enumerate((-1, 1)):
        @pl.when(jnp.logical_not(present(dr, 0)))
        def _():
            for seg in range(PASSES // MARGIN):
                for w in inner_order:
                    clear(far.at[seg, half, w], 0, MARGIN)
            for w in range(strips):
                clear(landed.at[half, w], 8, 8 + 4 * NEAR)
            for w in inner_order:
                first = end if half else top - MARGIN
                clear(route.at[w], first, first + MARGIN)

        for w, dc in ((left, -1), (right, 1)):
            @pl.when(jnp.logical_not(present(dr, dc)))
            def _():
                clear(landed.at[half, w], 8, 8 + 4 * NEAR)

    for w, dc in ((left, -1), (right, 1)):
        @pl.when(jnp.logical_not(present(0, dc)))
        def _():
            for a in range(4):
                clear(near.at[a, w], base, base + rows)

    def remote(side, src, dst, ssem, rsem):
        return side, pltpu.make_async_remote_copy(
            src_ref=src, dst_ref=dst, send_sem=ssem, recv_sem=rsem,
            device_id=(me_r + side[0], me_c + side[1]), device_id_type=MESH)

    def start_all(made):
        for (dr, dc), copy in made:
            pl.when(present(dr, dc))(lambda: copy.start())

    def arrive_all(made):
        for (dr, dc), copy in made:
            pl.when(present(-dr, -dc))(lambda: copy.wait_recv())

    def leave_all(made):
        for (dr, dc), copy in made:
            pl.when(present(dr, dc))(lambda: copy.wait_send())

    near_copies = []
    for d, (dr, dc) in enumerate(SIDES):
        if dr == 0:
            src = near.at[:, 0 if dc < 0 else strips - 1, own, :]
            dst = near.at[:, right if dc < 0 else left, own, :]
        else:
            half, at = (0 if dr < 0 else 1), pl.ds(8, 4 * NEAR)
            if dc == 0:
                src, dst = pack.at[half, :, at, :], landed.at[1 - half, pl.ds(0, strips), at, :]
            else:
                src = pack.at[half, 0 if dc < 0 else strips - 1, at, :]
                dst = landed.at[1 - half, right if dc < 0 else left, at, :]
        near_copies.append(remote((dr, dc), src, dst, near_ssem.at[d], near_rsem.at[d]))

    edge = {-1: (pl.ds(top, MARGIN), pl.ds(end, MARGIN)), 1: (pl.ds(end - MARGIN, MARGIN), pl.ds(top - MARGIN, MARGIN))}
    route_copies, route_mid_copies = [], []
    for d, (dr, dc) in enumerate(VERTICAL):
        source, target = edge[dr]
        route_copies.append(remote(
            (dr, dc), route.at[pl.ds(0, strips), source, :], route.at[pl.ds(0, strips), target, :],
            route_ssem.at[0, d], route_rsem.at[0, d]))
        route_mid_copies.append(remote(
            (dr, dc), route.at[mid, source, :], route.at[mid, target, :], route_ssem.at[1, d], route_rsem.at[1, d]))

    def far_copies(source, seg):
        return [
            remote((dr, dc), source.at[:, edge[dr][0], :], far.at[seg, 1 - d], far_ssem.at[seg, d], far_rsem.at[seg, d])
            for d, (dr, dc) in enumerate(VERTICAL)
        ]

    for load in loads:
        load.wait()
    for w in range(strips):
        for r in range(0, rows, 8):
            at, here = (pl.ds(r, 8), pl.ds(w * LANES, LANES)), pl.ds(base + r, 8)
            code = flow[at]
            kind = jnp.where(out_of[at] == 1, 0, code + 1).astype(jnp.float32)
            near[3, w, here, :] = kind
            route[w, pl.ds(top + r, 8), :] = kind
            length = jnp.where(code % 2 == 1, jnp.float32(0.70710678), jnp.float32(1.0))
            near[2, w, here, :] = plain[2, at[0], at[1]] * length
            for a in range(2):
                near[a, w, here, :] = plain[a, at[0], at[1]]
        for a in range(4):
            pack[0, w, pl.ds(8 + NEAR * a, 8), :] = near[a, w, pl.ds(base, 8), :]
        for a in reversed(range(4)):
            pack[1, w, pl.ds(8 + NEAR * (a - 1), 8), :] = near[a, w, pl.ds(base + rows - 8, 8), :]

    pl.semaphore_wait(barrier, neighbours)
    start_all(near_copies)
    start_all(route_copies)

    def make_masks(target, codes, w, r):
        around = {di: codes[w, pl.ds(r - di, 8), :] for di in (-1, 0, 1)}
        for k, (di, dj) in enumerate(OFFSETS):
            target[k, w, pl.ds(r, 8), :] = jnp.where(
                around[di] == jnp.float32(k + 1), jnp.float32(1.0), jnp.float32(0.0))

    def inflow(r):
        east, west, still = [], [], []
        here = pl.ds(r, 8)
        count = len(near_order)
        for w in near_order:
            x = {di: sent[w, pl.ds(r - di, 8), :] for di in (-1, 0, 1)}
            term = [near_masks[k, w, here, :] * x[di] for k, (di, _) in enumerate(OFFSETS)]
            east.append(term[0] + term[1] + term[7])
            west.append(term[3] + term[4] + term[5])
            still.append(rest[w, here, :] + term[2] + term[6])
        east = [pltpu.roll(x, 1, 1) for x in east]
        west = [pltpu.roll(x, LANES - 1, 1) for x in west]
        return [
            still[i]
            + jnp.where(lane == 0, east[i - 1], east[i])
            + jnp.where(lane == LANES - 1, west[(i + 1) % count], west[i])
            for i in range(count)
        ]

    def outflow(held, w, r):
        at = pl.ds(r, 8)
        h = held[w, at, :]
        factor = near[2, w, at, :] * jnp.exp2(jnp.log(h) * jnp.float32(2.0 / 3.0 / math.log(2.0)))
        out = h * (factor / (1.0 + factor))
        sent[w, at, :] = out
        rest[w, at, :] = h + near[1, w, at, :] - out

    for w in range(strips):
        for r in starts(base + 1, base + rows - 1):
            make_masks(near_masks, near.at[3], w, r)
        for r in range(base, base + rows, 8):
            outflow(near.at[0], w, r)

    arrive_all(near_copies)
    for r in range(0, rows, 8):
        here = pl.ds(base + r, 8)
        route[mid, pl.ds(top + r, 8), :] = jnp.where(lane < LANES // 2, near[3, right, here, :], near[3, left, here, :])
    start_all(route_mid_copies)
    for w in near_order:
        for a in range(4):
            near[a, w, pl.ds(base - 8, 8), :] = landed[0, w, pl.ds(8 + NEAR * (a - 1), 8), :]
            near[a, w, pl.ds(base + rows, 8), :] = landed[1, w, pl.ds(8 + NEAR * a, 8), :]

    reach = starts(base - NEAR, base + rows + NEAR)
    for w in near_order:
        for r in reach if w >= strips else (base - 7, base + rows - 1):
            make_masks(near_masks, near.at[3], w, r)
    for step in range(SUBSTEPS):
        for w in near_order:
            for r in (base - 8, base + rows) if step == 0 and w < strips else reach:
                outflow(near.at[0] if step == 0 else final, w, r)
        if step < SUBSTEPS - 1:
            for r in reach:
                for w, value in zip(near_order, inflow(r)):
                    final[w, pl.ds(r, 8), :] = value
    for r in range(0, rows, 8):
        new = inflow(base + r)
        for w in range(strips):
            new_depth[pl.ds(r, 8), pl.ds(w * LANES, LANES)] = new[1 + w]
            final[w, pl.ds(base + r, 8), :] = new[1 + w]
        final[mid, pl.ds(base + r, 8), :] = jnp.where(lane < LANES // 2, new[-1], new[0])

    def level_ring(step, carry):
        for half in range(0, rows // 2, 8):
            r = pl.multiple_of(step * (rows // 2), 8) + half
            for w, value in enumerate(to_ring([final[w, pl.ds(base + r, 8), :] for w in inner_order])):
                level[w, pl.ds(top + r, 8), :] = value
                state[0, w, pl.ds(top + r, 8), :] = value
        return carry

    lax.fori_loop(0, 2, level_ring, 0)
    start_all(far_copies(level, 0))

    def ring_routes(first, last):
        for r in range(first, last, 8):
            for w, value in enumerate(to_ring([route[w, pl.ds(r, 8), :] for w in inner_order])):
                ring_route[w, pl.ds(r, 8), :] = value

    ring_routes(top, end)
    for w in inner_order:
        for r in starts(top + 1, end - 1):
            make_masks(masks, ring_route, w, r)

    def one_pass(p, blocks):
        for r in blocks:
            here = pl.ds(r, 8)
            x = {di: state[p, :, pl.ds(r - di, 8), :] for di in (-1, 0, 1)}
            term = [masks[k, :, here, :] * x[di] for k, (di, _) in enumerate(OFFSETS)]
            east = term[0] + term[1] + term[7]
            west = term[3] + term[4] + term[5]
            still = level[:, here, :] + term[2] + term[6]
            east = jnp.concatenate([pltpu.roll(east[strips:], 1, 2), east[:strips]], axis=0)
            west = jnp.concatenate([west[1:], pltpu.roll(west[:1], LANES - 1, 2)], axis=0)
            value = still + east + west
            state[p + 1, :, here, :] = value
            if p == MARGIN - 1:
                state[0, :, here, :] = value

    def halo(seg, half):
        first = end if half else top - MARGIN
        for w in inner_order:
            for r in range(0, MARGIN, 8):
                state[0, w, pl.ds(first + r, 8), :] = far[seg, half, w, pl.ds(r, 8), :]

        @pl.when(seg == 0)
        def _():
            for w in inner_order:
                for r in range(0, MARGIN, 8):
                    level[w, pl.ds(first + r, 8), :] = far[0, half, w, pl.ds(r, 8), :]

    def bands():
        for p in range(MARGIN):
            one_pass(p, starts(top - MARGIN + p + 1, top + p + 1) + starts(end - p - 1, end + MARGIN - p - 1))

    def segment(seg, carry):
        for p in range(rows // 2 - 1):
            here, stop = top + p + 1, end - p - 1
            one_pass(p, starts(here, stop) if stop - here >= 8 else [here + (stop - here) // 2 - 4])

        @pl.when(seg == 0)
        def _():
            arrive_all(route_copies)
            arrive_all(route_mid_copies)
            ring_routes(top - MARGIN, top)
            ring_routes(end, end + MARGIN)
            for w in inner_order:
                for r in (*range(top - MARGIN, top + 8, 8), *range(end - 8, end + MARGIN, 8)):
                    make_masks(masks, ring_route, w, r)

        arrive_all(far_copies(level, seg))
        leave_all(far_copies(level, seg))
        halo(seg, 0)
        halo(seg, 1)
        bands()

        @pl.when(seg == 0)
        def _():
            start_all(far_copies(state.at[MARGIN], 1))

        return carry

    lax.fori_loop(0, PASSES // MARGIN, segment, 0)

    for w in inner_order:
        for r in range(0, rows, 8):
            runoff[w, pl.ds(r, 8), :] = state[MARGIN, w, pl.ds(top + r, 8), :]
    leave_all(near_copies)
    leave_all(route_copies)
    leave_all(route_mid_copies)


def finish(level, runoff, new_depth, discharge, logs, sems):
    first = pltpu.make_async_copy(level, new_depth, sems.at[0])
    first.start()
    rows, cols = level.shape
    made = [first]
    for part in range(4):
        for r in range(part * rows // 4, (part + 1) * rows // 4, 8):
            ring = [jnp.log(1.0 + runoff[w, pl.ds(r, 8), :]) for w in range(runoff.shape[0])]
            for w in range(cols // LANES):
                logs[pl.ds(r, 8), pl.ds(w * LANES, LANES)] = from_ring(ring, w)
        at = pl.ds(part * rows // 4, rows // 4)
        made.append(pltpu.make_async_copy(logs.at[at, :], discharge.at[at, :], sems.at[1 + part]))
        made[-1].start()
    for copy in made:
        copy.wait()


def solution(mesh):
    nrow, ncol = mesh.shape["row"], mesh.shape["col"]

    def on_device(depth, rainfall, conveyance, flow_dir, outlet):
        rows, cols = depth.shape
        strips = cols // LANES
        high = rows + 2 * MARGIN + 16
        low = rows + 32
        f32 = functools.partial(pltpu.VMEM, dtype=jnp.float32)
        dma = pltpu.SemaphoreType.DMA
        segments = PASSES // MARGIN
        pin = lambda x: pltpu.with_memory_space_constraint(x, pltpu.HBM)
        depth, rainfall, conveyance, flow_dir, outlet = map(pin, (depth, rainfall, conveyance, flow_dir, outlet))
        level, runoff = pl.pallas_call(
            functools.partial(kernel, rows, cols, nrow, ncol),
            out_shape=[
                jax.ShapeDtypeStruct((rows, cols), jnp.float32),
                jax.ShapeDtypeStruct((strips + 1, rows, LANES), jnp.float32),
            ],
            in_specs=[pl.BlockSpec(memory_space=pl.ANY)] * 5,
            out_specs=[pl.BlockSpec(memory_space=pltpu.VMEM)] * 2,
            scratch_shapes=[
                f32((4, strips + 3, low, LANES)),
                f32((3, rows, cols)),
                pltpu.VMEM((rows, cols), jnp.int32),
                pltpu.VMEM((rows, cols), jnp.int32),
                f32((2, strips, 32, LANES)),
                f32((2, strips + 3, 32, LANES)),
                f32((strips + 1, high, LANES)),
                f32((strips + 1, high, LANES)),
                f32((strips + 1, high, LANES)),
                f32((strips + 3, low, LANES)),
                f32((strips + 3, low, LANES)),
                f32((8, strips + 3, low, LANES)),
                f32((8, strips + 1, high, LANES)),
                f32((MARGIN + 1, strips + 1, high, LANES)),
                f32((segments, 2, strips + 1, MARGIN, LANES)),
                f32((strips + 3, low, LANES)),
                dma((5,)),
                dma((8,)), dma((8,)), dma((2, 2)), dma((2, 2)),
                dma((segments, 2)), dma((segments, 2)),
            ],
            compiler_params=pltpu.CompilerParams(
                collective_id=0, has_side_effects=True, vmem_limit_bytes=32 * 2**20),
            name="overland",
        )(depth, rainfall, conveyance, flow_dir, outlet)
        return tuple(pl.pallas_call(
            finish,
            out_shape=[jax.ShapeDtypeStruct((rows, cols), jnp.float32)] * 2,
            in_specs=[pl.BlockSpec(memory_space=pltpu.VMEM)] * 2,
            out_specs=[pl.BlockSpec(memory_space=pl.ANY)] * 2,
            scratch_shapes=[f32((rows, cols)), dma((5,))],
            compiler_params=pltpu.CompilerParams(vmem_limit_bytes=4 * 2**20),
            name="finish",
        )(level, runoff))

    placed = P("row", "col")
    return jax.shard_map(
        on_device, mesh=mesh, in_specs=(placed,) * 5, out_specs=(placed, placed), check_vma=False)
```

```python
import functools
import math

import jax
import jax.numpy as jnp
from jax import lax
from jax.experimental import pallas as pl
from jax.experimental.pallas import tpu as pltpu
from jax.sharding import PartitionSpec as P

SUBSTEPS = 3
PASSES = 64
MARGIN = 32
LANES = 128
NEAR = 4
MESH = pl.DeviceIdType.MESH
OFFSETS = ((0, 1), (1, 1), (1, 0), (1, -1), (0, -1), (-1, -1), (-1, 0), (-1, 1))
SIDES = ((-1, 0), (1, 0), (0, -1), (0, 1), (-1, -1), (-1, 1), (1, -1), (1, 1))
VERTICAL = ((-1, 0), (1, 0))


def starts(first, last):
    made = list(range(first, last - 7, 8))
    if made[-1] + 8 < last:
        made.append(last - 8)
    return made


def to_ring(values):
    count = len(values)
    lane = lax.broadcasted_iota(jnp.int32, values[0].shape, 1)
    made = []
    for w in range(count):
        n = count * lane + w
        at = n & (LANES - 1)
        out = jnp.take_along_axis(values[0], at, axis=1)
        for k in range(1, count):
            out = jnp.where(n >= k * LANES, jnp.take_along_axis(values[k], at, axis=1), out)
        made.append(out)
    return made


def from_ring(values, strip):
    count = len(values)
    n = lax.broadcasted_iota(jnp.int32, values[0].shape, 1) + strip * LANES
    at = (n * ((1 << 18) // count + 1)) >> 18
    which = n - count * at
    out = jnp.take_along_axis(values[0], at, axis=1)
    for k in range(1, count):
        out = jnp.where(which == k, jnp.take_along_axis(values[k], at, axis=1), out)
    return out


def kernel(
    rows, cols, nrow, ncol,
    depth, rainfall, conveyance, flow_dir, outlet, new_depth, runoff,
    near, plain, flow, out_of, pack, landed, route, ring_route, level, sent, rest, near_masks, masks, state, far, final,
    in_sem, near_ssem, near_rsem, route_ssem, route_rsem, far_ssem, far_rsem,
):
    strips = cols // LANES
    mid, left, right = strips, strips + 1, strips + 2
    inner_order = list(range(strips)) + [mid]
    near_order = [left] + list(range(strips)) + [right]
    top = MARGIN + 8
    end = top + rows
    base = 16
    me_r, me_c = lax.axis_index("row"), lax.axis_index("col")
    lane = lax.broadcasted_iota(jnp.int32, (8, LANES), 1)
    zero = jnp.zeros((8, LANES), jnp.float32)
    own = pl.ds(base, rows)

    def present(dr, dc):
        r, c = me_r + dr, me_c + dc
        return (r >= 0) & (r < nrow) & (c >= 0) & (c < ncol)

    barrier = pltpu.get_barrier_semaphore()
    neighbours = jnp.int32(0)
    for dr, dc in SIDES:
        here = present(dr, dc)
        neighbours = neighbours + here.astype(jnp.int32)

        @pl.when(here)
        def _():
            pl.semaphore_signal(barrier, inc=1, device_id=(me_r + dr, me_c + dc), device_id_type=MESH)

    loads = [
        pltpu.make_async_copy(source, target, in_sem.at[a])
        for a, (source, target) in enumerate((
            (flow_dir, flow), (outlet, out_of), (conveyance, plain.at[2]), (depth, plain.at[0]), (rainfall, plain.at[1]),
        ))
    ]
    for load in loads:
        load.start()

    def clear(ref, first, last):
        for r in range(first, last, 8):
            ref[pl.ds(r, 8), :] = zero

    for half, dr in enumerate((-1, 1)):
        @pl.when(jnp.logical_not(present(dr, 0)))
        def _():
            for seg in range(PASSES // MARGIN):
                for w in inner_order:
                    clear(far.at[seg, half, w], 0, MARGIN)
            for w in range(strips):
                clear(landed.at[half, w], 8, 8 + 4 * NEAR)
            for w in inner_order:
                first = end if half else top - MARGIN
                clear(route.at[w], first, first + MARGIN)

        for w, dc in ((left, -1), (right, 1)):
            @pl.when(jnp.logical_not(present(dr, dc)))
            def _():
                clear(landed.at[half, w], 8, 8 + 4 * NEAR)

    for w, dc in ((left, -1), (right, 1)):
        @pl.when(jnp.logical_not(present(0, dc)))
        def _():
            for a in range(4):
                clear(near.at[a, w], base, base + rows)

    def remote(side, src, dst, ssem, rsem):
        return side, pltpu.make_async_remote_copy(
            src_ref=src, dst_ref=dst, send_sem=ssem, recv_sem=rsem,
            device_id=(me_r + side[0], me_c + side[1]), device_id_type=MESH)

    def start_all(made):
        for (dr, dc), copy in made:
            pl.when(present(dr, dc))(lambda: copy.start())

    def arrive_all(made):
        for (dr, dc), copy in made:
            pl.when(present(-dr, -dc))(lambda: copy.wait_recv())

    def leave_all(made):
        for (dr, dc), copy in made:
            pl.when(present(dr, dc))(lambda: copy.wait_send())

    near_copies = []
    for d, (dr, dc) in enumerate(SIDES):
        if dr == 0:
            src = near.at[:, 0 if dc < 0 else strips - 1, own, :]
            dst = near.at[:, right if dc < 0 else left, own, :]
        else:
            half, at = (0 if dr < 0 else 1), pl.ds(8, 4 * NEAR)
            if dc == 0:
                src, dst = pack.at[half, :, at, :], landed.at[1 - half, pl.ds(0, strips), at, :]
            else:
                src = pack.at[half, 0 if dc < 0 else strips - 1, at, :]
                dst = landed.at[1 - half, right if dc < 0 else left, at, :]
        near_copies.append(remote((dr, dc), src, dst, near_ssem.at[d], near_rsem.at[d]))

    edge = {-1: (pl.ds(top, MARGIN), pl.ds(end, MARGIN)), 1: (pl.ds(end - MARGIN, MARGIN), pl.ds(top - MARGIN, MARGIN))}
    route_copies, route_mid_copies = [], []
    for d, (dr, dc) in enumerate(VERTICAL):
        source, target = edge[dr]
        route_copies.append(remote(
            (dr, dc), route.at[pl.ds(0, strips), source, :], route.at[pl.ds(0, strips), target, :],
            route_ssem.at[0, d], route_rsem.at[0, d]))
        route_mid_copies.append(remote(
            (dr, dc), route.at[mid, source, :], route.at[mid, target, :], route_ssem.at[1, d], route_rsem.at[1, d]))

    def far_copies(source, seg):
        return [
            remote((dr, dc), source.at[:, edge[dr][0], :], far.at[seg, 1 - d], far_ssem.at[seg, d], far_rsem.at[seg, d])
            for d, (dr, dc) in enumerate(VERTICAL)
        ]

    for load in loads:
        load.wait()
    for w in range(strips):
        for r in range(0, rows, 8):
            at, here = (pl.ds(r, 8), pl.ds(w * LANES, LANES)), pl.ds(base + r, 8)
            code = flow[at]
            kind = jnp.where(out_of[at] == 1, 0, code + 1).astype(jnp.float32)
            near[3, w, here, :] = kind
            route[w, pl.ds(top + r, 8), :] = kind
            length = jnp.where(code % 2 == 1, jnp.float32(0.70710678), jnp.float32(1.0))
            near[2, w, here, :] = plain[2, at[0], at[1]] * length
            for a in range(2):
                near[a, w, here, :] = plain[a, at[0], at[1]]
        for a in range(4):
            pack[0, w, pl.ds(8 + NEAR * a, 8), :] = near[a, w, pl.ds(base, 8), :]
        for a in reversed(range(4)):
            pack[1, w, pl.ds(8 + NEAR * (a - 1), 8), :] = near[a, w, pl.ds(base + rows - 8, 8), :]

    pl.semaphore_wait(barrier, neighbours)
    start_all(near_copies)
    start_all(route_copies)

    def make_masks(target, codes, w, r):
        around = {di: codes[w, pl.ds(r - di, 8), :] for di in (-1, 0, 1)}
        for k, (di, dj) in enumerate(OFFSETS):
            target[k, w, pl.ds(r, 8), :] = jnp.where(
                around[di] == jnp.float32(k + 1), jnp.float32(1.0), jnp.float32(0.0))

    def inflow(r):
        east, west, still = [], [], []
        here = pl.ds(r, 8)
        count = len(near_order)
        for w in near_order:
            x = {di: sent[w, pl.ds(r - di, 8), :] for di in (-1, 0, 1)}
            term = [near_masks[k, w, here, :] * x[di] for k, (di, _) in enumerate(OFFSETS)]
            east.append(term[0] + term[1] + term[7])
            west.append(term[3] + term[4] + term[5])
            still.append(rest[w, here, :] + term[2] + term[6])
        east = [pltpu.roll(x, 1, 1) for x in east]
        west = [pltpu.roll(x, LANES - 1, 1) for x in west]
        return [
            still[i]
            + jnp.where(lane == 0, east[i - 1], east[i])
            + jnp.where(lane == LANES - 1, west[(i + 1) % count], west[i])
            for i in range(count)
        ]

    def outflow(held, w, r):
        at = pl.ds(r, 8)
        h = held[w, at, :]
        factor = near[2, w, at, :] * jnp.exp2(jnp.log(h) * jnp.float32(2.0 / 3.0 / math.log(2.0)))
        out = h * (factor / (1.0 + factor))
        sent[w, at, :] = out
        rest[w, at, :] = h + near[1, w, at, :] - out

    for w in range(strips):
        for r in starts(base + 1, base + rows - 1):
            make_masks(near_masks, near.at[3], w, r)
        for r in range(base, base + rows, 8):
            outflow(near.at[0], w, r)

    arrive_all(near_copies)
    for r in range(0, rows, 8):
        here = pl.ds(base + r, 8)
        route[mid, pl.ds(top + r, 8), :] = jnp.where(lane < LANES // 2, near[3, right, here, :], near[3, left, here, :])
    start_all(route_mid_copies)
    for w in near_order:
        for a in range(4):
            near[a, w, pl.ds(base - 8, 8), :] = landed[0, w, pl.ds(8 + NEAR * (a - 1), 8), :]
            near[a, w, pl.ds(base + rows, 8), :] = landed[1, w, pl.ds(8 + NEAR * a, 8), :]

    reach = starts(base - NEAR, base + rows + NEAR)
    for w in near_order:
        for r in reach if w >= strips else (base - 7, base + rows - 1):
            make_masks(near_masks, near.at[3], w, r)
    for step in range(SUBSTEPS):
        for w in near_order:
            for r in (base - 8, base + rows) if step == 0 and w < strips else reach:
                outflow(near.at[0] if step == 0 else final, w, r)
        if step < SUBSTEPS - 1:
            for r in reach:
                for w, value in zip(near_order, inflow(r)):
                    final[w, pl.ds(r, 8), :] = value
    for r in range(0, rows, 8):
        new = inflow(base + r)
        for w in range(strips):
            new_depth[pl.ds(r, 8), pl.ds(w * LANES, LANES)] = new[1 + w]
            final[w, pl.ds(base + r, 8), :] = new[1 + w]
        final[mid, pl.ds(base + r, 8), :] = jnp.where(lane < LANES // 2, new[-1], new[0])

    @pl.when(me_r >= 0)
    def _():
        for r in range(0, rows, 8):
            for w, value in enumerate(to_ring([final[w, pl.ds(base + r, 8), :] for w in inner_order])):
                level[w, pl.ds(top + r, 8), :] = value
                state[0, w, pl.ds(top + r, 8), :] = value

    start_all(far_copies(level, 0))

    def ring_routes(first, last):
        for r in range(first, last, 8):
            for w, value in enumerate(to_ring([route[w, pl.ds(r, 8), :] for w in inner_order])):
                ring_route[w, pl.ds(r, 8), :] = value

    ring_routes(top, end)
    for w in inner_order:
        for r in starts(top + 1, end - 1):
            make_masks(masks, ring_route, w, r)

    sub = lax.broadcasted_iota(jnp.int32, (strips + 1, 8, LANES), 1)

    def down(x, before, n):
        return jnp.where(sub < n, pltpu.roll(before, n, 1), pltpu.roll(x, n, 1))

    def up(x, after, n):
        return jnp.where(sub < 8 - n, pltpu.roll(x, 8 - n, 1), pltpu.roll(after, 8 - n, 1))

    def flow_into(x, r):
        here = pl.ds(r, 8)
        term = [masks[k, :, here, :] * x[di] for k, (di, _) in enumerate(OFFSETS)]
        east = term[0] + term[1] + term[7]
        west = term[3] + term[4] + term[5]
        still = level[:, here, :] + term[2] + term[6]
        east = jnp.concatenate([pltpu.roll(east[strips:], 1, 2), east[:strips]], axis=0)
        west = jnp.concatenate([west[1:], pltpu.roll(west[:1], LANES - 1, 2)], axis=0)
        return still + east + west

    def one_pass(p, blocks):
        made = []
        for r in blocks:
            made.append(flow_into({di: state[p, :, pl.ds(r - di, 8), :] for di in (-1, 0, 1)}, r))
            state[p + 1, :, pl.ds(r, 8), :] = made[-1]
        return made

    def interior():
        for p in range(rows // 4 - 1):
            one_pass(p, starts(top + p + 1, end - p - 1))
        for first in range(rows // 4 - 1, rows // 2 - 1, 4):
            blocks = list(range(top + first + 1, end - first - 1, 8))
            held = one_pass(first, blocks)
            for p in range(first + 1, first + 4):
                new = []
                for b, r in enumerate(blocks):
                    new.append(flow_into({
                        1: down(held[b], held[max(b - 1, 0)], 1),
                        0: held[b],
                        -1: up(held[b], held[min(b + 1, len(held) - 1)], 1),
                    }, r))
                    state[p + 1, :, pl.ds(r, 8), :] = new[-1]
                held = new

    def finish_band(held, first):
        for b, value in enumerate(held):
            for s in (0, MARGIN):
                state[s, :, pl.ds(first + 8 * b, 8), :] = value

    def top_band(seg):
        arrive_all(far_copies(level, seg)[1:])
        copy_level(seg, 0, top - MARGIN)
        held = [far[seg, 0, :, pl.ds(r, 8), :] for r in range(0, MARGIN, 8)]
        for p in range(MARGIN):
            held.append(state[p, :, pl.ds(top + p, 8), :])
            new = []
            for b in range(MARGIN // 8):
                new.append(flow_into({
                    1: held[b], 0: up(held[b], held[b + 1], 1), -1: up(held[b], held[b + 1], 2),
                }, top - MARGIN + p + 1 + 8 * b))
            held = new
        finish_band(held, top)

    def bottom_band(seg):
        arrive_all(far_copies(level, seg)[:1])
        copy_level(seg, 1, end)
        held = [far[seg, 1, :, pl.ds(r, 8), :] for r in range(0, MARGIN, 8)]
        for p in range(MARGIN):
            held.insert(0, state[p, :, pl.ds(end - p - 8, 8), :])
            new = []
            for b in range(MARGIN // 8):
                new.append(flow_into({
                    1: down(held[b + 1], held[b], 2), 0: down(held[b + 1], held[b], 1), -1: held[b + 1],
                }, end - p - 1 + 8 * b))
            held = new
        finish_band(held, end - MARGIN)

    def copy_level(seg, half, first):
        @pl.when(seg == 0)
        def _():
            for r in range(0, MARGIN, 8):
                level[:, pl.ds(first + r, 8), :] = far[0, half, :, pl.ds(r, 8), :]

    def segment(seg, carry):
        interior()

        @pl.when(seg == 0)
        def _():
            arrive_all(route_copies)
            arrive_all(route_mid_copies)
            ring_routes(top - MARGIN, top)
            ring_routes(end, end + MARGIN)
            for w in inner_order:
                for r in (*range(top - MARGIN, top + 8, 8), *range(end - 8, end + MARGIN, 8)):
                    make_masks(masks, ring_route, w, r)
            top_band(0)
            start_all(far_copies(state.at[MARGIN], 1)[:1])

        leave_all(far_copies(level, seg))
        bottom_band(seg)

        @pl.when(seg == 0)
        def _():
            start_all(far_copies(state.at[MARGIN], 1)[1:])

        @pl.when(seg == 1)
        def _():
            top_band(1)

        return carry

    lax.fori_loop(0, PASSES // MARGIN, segment, 0)

    for w in inner_order:
        for r in range(0, rows, 8):
            runoff[w, pl.ds(r, 8), :] = state[MARGIN, w, pl.ds(top + r, 8), :]
    leave_all(near_copies)
    leave_all(route_copies)
    leave_all(route_mid_copies)


def finish(level, runoff, new_depth, discharge, logs, sems):
    first = pltpu.make_async_copy(level, new_depth, sems.at[0])
    first.start()
    rows, cols = level.shape
    made = [first]
    for part in range(4):
        for r in range(part * rows // 4, (part + 1) * rows // 4, 8):
            ring = [jnp.log(1.0 + runoff[w, pl.ds(r, 8), :]) for w in range(runoff.shape[0])]
            for w in range(cols // LANES):
                logs[pl.ds(r, 8), pl.ds(w * LANES, LANES)] = from_ring(ring, w)
        at = pl.ds(part * rows // 4, rows // 4)
        made.append(pltpu.make_async_copy(logs.at[at, :], discharge.at[at, :], sems.at[1 + part]))
        made[-1].start()
    for copy in made:
        copy.wait()


def solution(mesh):
    nrow, ncol = mesh.shape["row"], mesh.shape["col"]

    def on_device(depth, rainfall, conveyance, flow_dir, outlet):
        rows, cols = depth.shape
        strips = cols // LANES
        high = rows + 2 * MARGIN + 16
        low = rows + 32
        f32 = functools.partial(pltpu.VMEM, dtype=jnp.float32)
        dma = pltpu.SemaphoreType.DMA
        segments = PASSES // MARGIN
        pin = lambda x: pltpu.with_memory_space_constraint(x, pltpu.HBM)
        depth, rainfall, conveyance, flow_dir, outlet = map(pin, (depth, rainfall, conveyance, flow_dir, outlet))
        level, runoff = pl.pallas_call(
            functools.partial(kernel, rows, cols, nrow, ncol),
            out_shape=[
                jax.ShapeDtypeStruct((rows, cols), jnp.float32),
                jax.ShapeDtypeStruct((strips + 1, rows, LANES), jnp.float32),
            ],
            in_specs=[pl.BlockSpec(memory_space=pl.ANY)] * 5,
            out_specs=[pl.BlockSpec(memory_space=pltpu.VMEM)] * 2,
            scratch_shapes=[
                f32((4, strips + 3, low, LANES)),
                f32((3, rows, cols)),
                pltpu.VMEM((rows, cols), jnp.int32),
                pltpu.VMEM((rows, cols), jnp.int32),
                f32((2, strips, 32, LANES)),
                f32((2, strips + 3, 32, LANES)),
                f32((strips + 1, high, LANES)),
                f32((strips + 1, high, LANES)),
                f32((strips + 1, high, LANES)),
                f32((strips + 3, low, LANES)),
                f32((strips + 3, low, LANES)),
                f32((8, strips + 3, low, LANES)),
                f32((8, strips + 1, high, LANES)),
                f32((MARGIN + 1, strips + 1, high, LANES)),
                f32((segments, 2, strips + 1, MARGIN, LANES)),
                f32((strips + 3, low, LANES)),
                dma((5,)),
                dma((8,)), dma((8,)), dma((2, 2)), dma((2, 2)),
                dma((segments, 2)), dma((segments, 2)),
            ],
            compiler_params=pltpu.CompilerParams(
                collective_id=0, has_side_effects=True, vmem_limit_bytes=32 * 2**20),
            name="overland",
        )(depth, rainfall, conveyance, flow_dir, outlet)
        return tuple(pl.pallas_call(
            finish,
            out_shape=[jax.ShapeDtypeStruct((rows, cols), jnp.float32)] * 2,
            in_specs=[pl.BlockSpec(memory_space=pltpu.VMEM)] * 2,
            out_specs=[pl.BlockSpec(memory_space=pl.ANY)] * 2,
            scratch_shapes=[f32((rows, cols)), dma((5,))],
            compiler_params=pltpu.CompilerParams(vmem_limit_bytes=4 * 2**20),
            name="finish",
        )(level, runoff))

    placed = P("row", "col")
    return jax.shard_map(
        on_device, mesh=mesh, in_specs=(placed,) * 5, out_specs=(placed, placed), check_vma=False)
```

```python
import functools
import math

import jax
import jax.numpy as jnp
from jax import lax
from jax.experimental import pallas as pl
from jax.experimental.pallas import tpu as pltpu
from jax.sharding import PartitionSpec as P

SUBSTEPS = 3
PASSES = 64
MARGIN = 32
LANES = 128
NEAR = 4
MESH = pl.DeviceIdType.MESH
OFFSETS = ((0, 1), (1, 1), (1, 0), (1, -1), (0, -1), (-1, -1), (-1, 0), (-1, 1))
SIDES = ((-1, 0), (1, 0), (0, -1), (0, 1), (-1, -1), (-1, 1), (1, -1), (1, 1))
VERTICAL = ((-1, 0), (1, 0))


def starts(first, last):
    made = list(range(first, last - 7, 8))
    if made[-1] + 8 < last:
        made.append(last - 8)
    return made


def to_ring(values):
    count = len(values)
    lane = lax.broadcasted_iota(jnp.int32, values[0].shape, 1)
    made = []
    for w in range(count):
        n = count * lane + w
        at = n & (LANES - 1)
        out = jnp.take_along_axis(values[0], at, axis=1)
        for k in range(1, count):
            out = jnp.where(n >= k * LANES, jnp.take_along_axis(values[k], at, axis=1), out)
        made.append(out)
    return made


def from_ring(values, strip):
    count = len(values)
    n = lax.broadcasted_iota(jnp.int32, values[0].shape, 1) + strip * LANES
    at = (n * ((1 << 18) // count + 1)) >> 18
    which = n - count * at
    out = jnp.take_along_axis(values[0], at, axis=1)
    for k in range(1, count):
        out = jnp.where(which == k, jnp.take_along_axis(values[k], at, axis=1), out)
    return out


def kernel(
    rows, cols, nrow, ncol,
    depth, rainfall, conveyance, flow_dir, outlet, new_depth, runoff,
    near, plain, flow, out_of, pack, landed, route, ring_route, level, sent, rest, near_masks, masks, state, far, final,
    in_sem, near_ssem, near_rsem, route_ssem, route_rsem, far_ssem, far_rsem,
):
    strips = cols // LANES
    mid, left, right = strips, strips + 1, strips + 2
    inner_order = list(range(strips)) + [mid]
    near_order = [left] + list(range(strips)) + [right]
    top = MARGIN + 8
    end = top + rows
    base = 16
    me_r, me_c = lax.axis_index("row"), lax.axis_index("col")
    lane = lax.broadcasted_iota(jnp.int32, (8, LANES), 1)
    zero = jnp.zeros((8, LANES), jnp.float32)
    own = pl.ds(base, rows)

    def present(dr, dc):
        r, c = me_r + dr, me_c + dc
        return (r >= 0) & (r < nrow) & (c >= 0) & (c < ncol)

    barrier = pltpu.get_barrier_semaphore()
    neighbours = jnp.int32(0)
    for dr, dc in SIDES:
        here = present(dr, dc)
        neighbours = neighbours + here.astype(jnp.int32)

        @pl.when(here)
        def _():
            pl.semaphore_signal(barrier, inc=1, device_id=(me_r + dr, me_c + dc), device_id_type=MESH)

    loads = [
        pltpu.make_async_copy(source, target, in_sem.at[a])
        for a, (source, target) in enumerate((
            (flow_dir, flow), (outlet, out_of), (conveyance, plain.at[2]), (depth, plain.at[0]), (rainfall, plain.at[1]),
        ))
    ]
    for load in loads:
        load.start()

    def clear(ref, first, last):
        for r in range(first, last, 8):
            ref[pl.ds(r, 8), :] = zero

    for half, dr in enumerate((-1, 1)):
        @pl.when(jnp.logical_not(present(dr, 0)))
        def _():
            for seg in range(PASSES // MARGIN):
                for w in inner_order:
                    clear(far.at[seg, half, w], 0, MARGIN)
            for w in range(strips):
                clear(landed.at[half, w], 8, 8 + 4 * NEAR)
            for w in inner_order:
                first = end if half else top - MARGIN
                clear(route.at[w], first, first + MARGIN)

        for w, dc in ((left, -1), (right, 1)):
            @pl.when(jnp.logical_not(present(dr, dc)))
            def _():
                clear(landed.at[half, w], 8, 8 + 4 * NEAR)

    for w, dc in ((left, -1), (right, 1)):
        @pl.when(jnp.logical_not(present(0, dc)))
        def _():
            for a in range(4):
                clear(near.at[a, w], base, base + rows)

    def remote(side, src, dst, ssem, rsem):
        return side, pltpu.make_async_remote_copy(
            src_ref=src, dst_ref=dst, send_sem=ssem, recv_sem=rsem,
            device_id=(me_r + side[0], me_c + side[1]), device_id_type=MESH)

    def start_all(made):
        for (dr, dc), copy in made:
            pl.when(present(dr, dc))(lambda: copy.start())

    def arrive_all(made):
        for (dr, dc), copy in made:
            pl.when(present(-dr, -dc))(lambda: copy.wait_recv())

    def leave_all(made):
        for (dr, dc), copy in made:
            pl.when(present(dr, dc))(lambda: copy.wait_send())

    near_copies = []
    for d, (dr, dc) in enumerate(SIDES):
        if dr == 0:
            src = near.at[:, 0 if dc < 0 else strips - 1, own, :]
            dst = near.at[:, right if dc < 0 else left, own, :]
        else:
            half, at = (0 if dr < 0 else 1), pl.ds(8, 4 * NEAR)
            if dc == 0:
                src, dst = pack.at[half, :, at, :], landed.at[1 - half, pl.ds(0, strips), at, :]
            else:
                src = pack.at[half, 0 if dc < 0 else strips - 1, at, :]
                dst = landed.at[1 - half, right if dc < 0 else left, at, :]
        near_copies.append(remote((dr, dc), src, dst, near_ssem.at[d], near_rsem.at[d]))

    edge = {-1: (pl.ds(top, MARGIN), pl.ds(end, MARGIN)), 1: (pl.ds(end - MARGIN, MARGIN), pl.ds(top - MARGIN, MARGIN))}
    route_copies, route_mid_copies = [], []
    for d, (dr, dc) in enumerate(VERTICAL):
        source, target = edge[dr]
        route_copies.append(remote(
            (dr, dc), route.at[pl.ds(0, strips), source, :], route.at[pl.ds(0, strips), target, :],
            route_ssem.at[0, d], route_rsem.at[0, d]))
        route_mid_copies.append(remote(
            (dr, dc), route.at[mid, source, :], route.at[mid, target, :], route_ssem.at[1, d], route_rsem.at[1, d]))

    def far_copies(source, seg):
        return [
            remote((dr, dc), source.at[:, edge[dr][0], :], far.at[seg, 1 - d], far_ssem.at[seg, d], far_rsem.at[seg, d])
            for d, (dr, dc) in enumerate(VERTICAL)
        ]

    for load in loads:
        load.wait()
    for w in range(strips):
        for r in range(0, rows, 8):
            at, here = (pl.ds(r, 8), pl.ds(w * LANES, LANES)), pl.ds(base + r, 8)
            code = flow[at]
            kind = jnp.where(out_of[at] == 1, 0, code + 1).astype(jnp.float32)
            near[3, w, here, :] = kind
            route[w, pl.ds(top + r, 8), :] = kind
            length = jnp.where(code % 2 == 1, jnp.float32(0.70710678), jnp.float32(1.0))
            near[2, w, here, :] = plain[2, at[0], at[1]] * length
            for a in range(2):
                near[a, w, here, :] = plain[a, at[0], at[1]]
        for a in range(4):
            pack[0, w, pl.ds(8 + NEAR * a, 8), :] = near[a, w, pl.ds(base, 8), :]
        for a in reversed(range(4)):
            pack[1, w, pl.ds(8 + NEAR * (a - 1), 8), :] = near[a, w, pl.ds(base + rows - 8, 8), :]

    pl.semaphore_wait(barrier, neighbours)
    start_all(near_copies)
    start_all(route_copies)

    def make_masks(target, codes, w, r):
        around = {di: codes[w, pl.ds(r - di, 8), :] for di in (-1, 0, 1)}
        for k, (di, dj) in enumerate(OFFSETS):
            target[k, w, pl.ds(r, 8), :] = jnp.where(
                around[di] == jnp.float32(k + 1), jnp.float32(1.0), jnp.float32(0.0))

    def inflow(r):
        east, west, still = [], [], []
        here = pl.ds(r, 8)
        count = len(near_order)
        for w in near_order:
            x = {di: sent[w, pl.ds(r - di, 8), :] for di in (-1, 0, 1)}
            term = [near_masks[k, w, here, :] * x[di] for k, (di, _) in enumerate(OFFSETS)]
            east.append(term[0] + term[1] + term[7])
            west.append(term[3] + term[4] + term[5])
            still.append(rest[w, here, :] + term[2] + term[6])
        east = [pltpu.roll(x, 1, 1) for x in east]
        west = [pltpu.roll(x, LANES - 1, 1) for x in west]
        return [
            still[i]
            + jnp.where(lane == 0, east[i - 1], east[i])
            + jnp.where(lane == LANES - 1, west[(i + 1) % count], west[i])
            for i in range(count)
        ]

    def outflow(held, w, r):
        at = pl.ds(r, 8)
        h = held[w, at, :]
        factor = near[2, w, at, :] * jnp.exp2(jnp.log(h) * jnp.float32(2.0 / 3.0 / math.log(2.0)))
        out = h * (factor / (1.0 + factor))
        sent[w, at, :] = out
        rest[w, at, :] = h + near[1, w, at, :] - out

    for w in range(strips):
        for r in starts(base + 1, base + rows - 1):
            make_masks(near_masks, near.at[3], w, r)
        for r in range(base, base + rows, 8):
            outflow(near.at[0], w, r)

    arrive_all(near_copies)
    for r in range(0, rows, 8):
        here = pl.ds(base + r, 8)
        route[mid, pl.ds(top + r, 8), :] = jnp.where(lane < LANES // 2, near[3, right, here, :], near[3, left, here, :])
    start_all(route_mid_copies)
    for w in near_order:
        for a in range(4):
            near[a, w, pl.ds(base - 8, 8), :] = landed[0, w, pl.ds(8 + NEAR * (a - 1), 8), :]
            near[a, w, pl.ds(base + rows, 8), :] = landed[1, w, pl.ds(8 + NEAR * a, 8), :]

    reach = starts(base - NEAR, base + rows + NEAR)
    for w in near_order:
        for r in reach if w >= strips else (base - 7, base + rows - 1):
            make_masks(near_masks, near.at[3], w, r)
    for step in range(SUBSTEPS):
        for w in near_order:
            for r in (base - 8, base + rows) if step == 0 and w < strips else reach:
                outflow(near.at[0] if step == 0 else final, w, r)
        if step < SUBSTEPS - 1:
            for r in reach:
                for w, value in zip(near_order, inflow(r)):
                    final[w, pl.ds(r, 8), :] = value
    for r in range(0, rows, 8):
        new = inflow(base + r)
        for w in range(strips):
            new_depth[pl.ds(r, 8), pl.ds(w * LANES, LANES)] = new[1 + w]
            final[w, pl.ds(base + r, 8), :] = new[1 + w]
        final[mid, pl.ds(base + r, 8), :] = jnp.where(lane < LANES // 2, new[-1], new[0])

    @pl.when(me_r >= 0)
    def _():
        for r in range(0, rows, 8):
            for w, value in enumerate(to_ring([final[w, pl.ds(base + r, 8), :] for w in inner_order])):
                level[w, pl.ds(top + r, 8), :] = value
                state[0, w, pl.ds(top + r, 8), :] = value

    start_all(far_copies(level, 0))

    def ring_routes(first, last):
        for r in range(first, last, 8):
            for w, value in enumerate(to_ring([route[w, pl.ds(r, 8), :] for w in inner_order])):
                ring_route[w, pl.ds(r, 8), :] = value

    ring_routes(top, end)
    for w in inner_order:
        for r in starts(top + 1, end - 1):
            make_masks(masks, ring_route, w, r)

    def one_pass(p, blocks):
        for r in blocks:
            here = pl.ds(r, 8)
            x = {di: state[p, :, pl.ds(r - di, 8), :] for di in (-1, 0, 1)}
            term = [masks[k, :, here, :] * x[di] for k, (di, _) in enumerate(OFFSETS)]
            east = term[0] + term[1] + term[7]
            west = term[3] + term[4] + term[5]
            still = level[:, here, :] + term[2] + term[6]
            east = jnp.concatenate([pltpu.roll(east[strips:], 1, 2), east[:strips]], axis=0)
            west = jnp.concatenate([west[1:], pltpu.roll(west[:1], LANES - 1, 2)], axis=0)
            value = still + east + west
            state[p + 1, :, here, :] = value
            if p == MARGIN - 1:
                state[0, :, here, :] = value

    def halo(seg, half):
        first = end if half else top - MARGIN
        for w in inner_order:
            for r in range(0, MARGIN, 8):
                state[0, w, pl.ds(first + r, 8), :] = far[seg, half, w, pl.ds(r, 8), :]

        @pl.when(seg == 0)
        def _():
            for w in inner_order:
                for r in range(0, MARGIN, 8):
                    level[w, pl.ds(first + r, 8), :] = far[0, half, w, pl.ds(r, 8), :]

    def bands():
        for p in range(MARGIN):
            one_pass(p, starts(top - MARGIN + p + 1, top + p + 1) + starts(end - p - 1, end + MARGIN - p - 1))

    def segment(seg, carry):
        for p in range(rows // 2 - 1):
            here, stop = top + p + 1, end - p - 1
            one_pass(p, starts(here, stop) if stop - here >= 8 else [here + (stop - here) // 2 - 4])

        @pl.when(seg == 0)
        def _():
            arrive_all(route_copies)
            arrive_all(route_mid_copies)
            ring_routes(top - MARGIN, top)
            ring_routes(end, end + MARGIN)
            for w in inner_order:
                for r in (*range(top - MARGIN, top + 8, 8), *range(end - 8, end + MARGIN, 8)):
                    make_masks(masks, ring_route, w, r)

        arrive_all(far_copies(level, seg))
        leave_all(far_copies(level, seg))
        halo(seg, 0)
        halo(seg, 1)
        bands()

        @pl.when(seg == 0)
        def _():
            start_all(far_copies(state.at[MARGIN], 1))

        return carry

    lax.fori_loop(0, PASSES // MARGIN, segment, 0)

    for w in inner_order:
        for r in range(0, rows, 8):
            runoff[w, pl.ds(r, 8), :] = state[MARGIN, w, pl.ds(top + r, 8), :]
    leave_all(near_copies)
    leave_all(route_copies)
    leave_all(route_mid_copies)


def finish(level, runoff, new_depth, discharge, logs, sems):
    first = pltpu.make_async_copy(level, new_depth, sems.at[0])
    first.start()
    rows, cols = level.shape
    made = [first]
    for part in range(4):
        for r in range(part * rows // 4, (part + 1) * rows // 4, 8):
            ring = [jnp.log(1.0 + runoff[w, pl.ds(r, 8), :]) for w in range(runoff.shape[0])]
            for w in range(cols // LANES):
                logs[pl.ds(r, 8), pl.ds(w * LANES, LANES)] = from_ring(ring, w)
        at = pl.ds(part * rows // 4, rows // 4)
        made.append(pltpu.make_async_copy(logs.at[at, :], discharge.at[at, :], sems.at[1 + part]))
        made[-1].start()
    for copy in made:
        copy.wait()


def solution(mesh):
    nrow, ncol = mesh.shape["row"], mesh.shape["col"]

    def on_device(depth, rainfall, conveyance, flow_dir, outlet):
        rows, cols = depth.shape
        strips = cols // LANES
        high = rows + 2 * MARGIN + 24
        low = rows + 40
        f32 = functools.partial(pltpu.VMEM, dtype=jnp.float32)
        dma = pltpu.SemaphoreType.DMA
        segments = PASSES // MARGIN
        pin = lambda x: pltpu.with_memory_space_constraint(x, pltpu.HBM)
        depth, rainfall, conveyance, flow_dir, outlet = map(pin, (depth, rainfall, conveyance, flow_dir, outlet))
        level, runoff = pl.pallas_call(
            functools.partial(kernel, rows, cols, nrow, ncol),
            out_shape=[
                jax.ShapeDtypeStruct((rows, cols), jnp.float32),
                jax.ShapeDtypeStruct((strips + 1, rows, LANES), jnp.float32),
            ],
            in_specs=[pl.BlockSpec(memory_space=pl.ANY)] * 5,
            out_specs=[pl.BlockSpec(memory_space=pltpu.VMEM)] * 2,
            scratch_shapes=[
                f32((4, strips + 3, low, LANES)),
                f32((3, rows, cols)),
                pltpu.VMEM((rows, cols), jnp.int32),
                pltpu.VMEM((rows, cols), jnp.int32),
                f32((2, strips, 32, LANES)),
                f32((2, strips + 3, 32, LANES)),
                f32((strips + 1, high, LANES)),
                f32((strips + 1, high, LANES)),
                f32((strips + 1, high, LANES)),
                f32((strips + 3, low, LANES)),
                f32((strips + 3, low, LANES)),
                f32((8, strips + 3, low, LANES)),
                f32((8, strips + 1, high, LANES)),
                f32((MARGIN + 1, strips + 1, high, LANES)),
                f32((segments, 2, strips + 1, MARGIN, LANES)),
                f32((strips + 3, low, LANES)),
                dma((5,)),
                dma((8,)), dma((8,)), dma((2, 2)), dma((2, 2)),
                dma((segments, 2)), dma((segments, 2)),
            ],
            compiler_params=pltpu.CompilerParams(
                collective_id=0, has_side_effects=True, vmem_limit_bytes=32 * 2**20),
            name="overland",
        )(depth, rainfall, conveyance, flow_dir, outlet)
        return tuple(pl.pallas_call(
            finish,
            out_shape=[jax.ShapeDtypeStruct((rows, cols), jnp.float32)] * 2,
            in_specs=[pl.BlockSpec(memory_space=pltpu.VMEM)] * 2,
            out_specs=[pl.BlockSpec(memory_space=pl.ANY)] * 2,
            scratch_shapes=[f32((rows, cols)), dma((5,))],
            compiler_params=pltpu.CompilerParams(vmem_limit_bytes=4 * 2**20),
            name="finish",
        )(level, runoff))

    placed = P("row", "col")
    return jax.shard_map(
        on_device, mesh=mesh, in_specs=(placed,) * 5, out_specs=(placed, placed), check_vma=False)
```

```python
import functools
import math

import jax
import jax.numpy as jnp
from jax import lax
from jax.experimental import pallas as pl
from jax.experimental.pallas import tpu as pltpu
from jax.sharding import PartitionSpec as P

SUBSTEPS = 3
PASSES = 64
MARGIN = 32
LANES = 128
NEAR = 4
MESH = pl.DeviceIdType.MESH
OFFSETS = ((0, 1), (1, 1), (1, 0), (1, -1), (0, -1), (-1, -1), (-1, 0), (-1, 1))
SIDES = ((-1, 0), (1, 0), (0, -1), (0, 1), (-1, -1), (-1, 1), (1, -1), (1, 1))
VERTICAL = ((-1, 0), (1, 0))


def starts(first, last):
    made = list(range(first, last - 7, 8))
    if made[-1] + 8 < last:
        made.append(last - 8)
    return made


def to_ring(values):
    count = len(values)
    lane = lax.broadcasted_iota(jnp.int32, values[0].shape, 1)
    made = []
    for w in range(count):
        n = count * lane + w
        at = n & (LANES - 1)
        out = jnp.take_along_axis(values[0], at, axis=1)
        for k in range(1, count):
            out = jnp.where(n >= k * LANES, jnp.take_along_axis(values[k], at, axis=1), out)
        made.append(out)
    return made


def from_ring(values, strip):
    count = len(values)
    n = lax.broadcasted_iota(jnp.int32, values[0].shape, 1) + strip * LANES
    at = (n * ((1 << 18) // count + 1)) >> 18
    which = n - count * at
    out = jnp.take_along_axis(values[0], at, axis=1)
    for k in range(1, count):
        out = jnp.where(which == k, jnp.take_along_axis(values[k], at, axis=1), out)
    return out


def kernel(
    rows, cols, nrow, ncol,
    depth, rainfall, conveyance, flow_dir, outlet, new_depth, runoff,
    near, plain, flow, out_of, pack, landed, route, ring_route, level, sent, rest, near_masks, masks, state, far, final,
    in_sem, near_ssem, near_rsem, route_ssem, route_rsem, far_ssem, far_rsem,
):
    strips = cols // LANES
    mid, left, right = strips, strips + 1, strips + 2
    inner_order = list(range(strips)) + [mid]
    near_order = [left] + list(range(strips)) + [right]
    top = MARGIN + 8
    end = top + rows
    base = 16
    me_r, me_c = lax.axis_index("row"), lax.axis_index("col")
    lane = lax.broadcasted_iota(jnp.int32, (8, LANES), 1)
    zero = jnp.zeros((8, LANES), jnp.float32)
    own = pl.ds(base, rows)

    def present(dr, dc):
        r, c = me_r + dr, me_c + dc
        return (r >= 0) & (r < nrow) & (c >= 0) & (c < ncol)

    barrier = pltpu.get_barrier_semaphore()
    neighbours = jnp.int32(0)
    for dr, dc in SIDES:
        here = present(dr, dc)
        neighbours = neighbours + here.astype(jnp.int32)

        @pl.when(here)
        def _():
            pl.semaphore_signal(barrier, inc=1, device_id=(me_r + dr, me_c + dc), device_id_type=MESH)

    loads = [
        pltpu.make_async_copy(source, target, in_sem.at[a])
        for a, (source, target) in enumerate((
            (flow_dir, flow), (outlet, out_of), (conveyance, plain.at[2]), (depth, plain.at[0]), (rainfall, plain.at[1]),
        ))
    ]
    for load in loads:
        load.start()

    def clear(ref, first, last):
        for r in range(first, last, 8):
            ref[pl.ds(r, 8), :] = zero

    for half, dr in enumerate((-1, 1)):
        @pl.when(jnp.logical_not(present(dr, 0)))
        def _():
            for seg in range(PASSES // MARGIN):
                for w in inner_order:
                    clear(far.at[seg, half, w], 0, MARGIN)
            for w in range(strips):
                clear(landed.at[half, w], 8, 8 + 4 * NEAR)
            for w in inner_order:
                first = end if half else top - MARGIN
                clear(route.at[w], first, first + MARGIN)

        for w, dc in ((left, -1), (right, 1)):
            @pl.when(jnp.logical_not(present(dr, dc)))
            def _():
                clear(landed.at[half, w], 8, 8 + 4 * NEAR)

    for w, dc in ((left, -1), (right, 1)):
        @pl.when(jnp.logical_not(present(0, dc)))
        def _():
            for a in range(4):
                clear(near.at[a, w], base, base + rows)

    def remote(side, src, dst, ssem, rsem):
        return side, pltpu.make_async_remote_copy(
            src_ref=src, dst_ref=dst, send_sem=ssem, recv_sem=rsem,
            device_id=(me_r + side[0], me_c + side[1]), device_id_type=MESH)

    def start_all(made):
        for (dr, dc), copy in made:
            pl.when(present(dr, dc))(lambda: copy.start())

    def arrive_all(made):
        for (dr, dc), copy in made:
            pl.when(present(-dr, -dc))(lambda: copy.wait_recv())

    def leave_all(made):
        for (dr, dc), copy in made:
            pl.when(present(dr, dc))(lambda: copy.wait_send())

    near_copies = []
    for d, (dr, dc) in enumerate(SIDES):
        if dr == 0:
            src = near.at[:, 0 if dc < 0 else strips - 1, own, :]
            dst = near.at[:, right if dc < 0 else left, own, :]
        else:
            half, at = (0 if dr < 0 else 1), pl.ds(8, 4 * NEAR)
            if dc == 0:
                src, dst = pack.at[half, :, at, :], landed.at[1 - half, pl.ds(0, strips), at, :]
            else:
                src = pack.at[half, 0 if dc < 0 else strips - 1, at, :]
                dst = landed.at[1 - half, right if dc < 0 else left, at, :]
        near_copies.append(remote((dr, dc), src, dst, near_ssem.at[d], near_rsem.at[d]))

    edge = {-1: (pl.ds(top, MARGIN), pl.ds(end, MARGIN)), 1: (pl.ds(end - MARGIN, MARGIN), pl.ds(top - MARGIN, MARGIN))}
    route_copies, route_mid_copies = [], []
    for d, (dr, dc) in enumerate(VERTICAL):
        source, target = edge[dr]
        route_copies.append(remote(
            (dr, dc), route.at[pl.ds(0, strips), source, :], route.at[pl.ds(0, strips), target, :],
            route_ssem.at[0, d], route_rsem.at[0, d]))
        route_mid_copies.append(remote(
            (dr, dc), route.at[mid, source, :], route.at[mid, target, :], route_ssem.at[1, d], route_rsem.at[1, d]))

    def far_copies(source, seg):
        return [
            remote((dr, dc), source.at[:, edge[dr][0], :], far.at[seg, 1 - d], far_ssem.at[seg, d], far_rsem.at[seg, d])
            for d, (dr, dc) in enumerate(VERTICAL)
        ]

    for load in loads:
        load.wait()
    for w in range(strips):
        for r in range(0, rows, 8):
            at, here = (pl.ds(r, 8), pl.ds(w * LANES, LANES)), pl.ds(base + r, 8)
            code = flow[at]
            kind = jnp.where(out_of[at] == 1, 0, code + 1).astype(jnp.float32)
            near[3, w, here, :] = kind
            route[w, pl.ds(top + r, 8), :] = kind
            length = jnp.where(code % 2 == 1, jnp.float32(0.70710678), jnp.float32(1.0))
            near[2, w, here, :] = plain[2, at[0], at[1]] * length
            for a in range(2):
                near[a, w, here, :] = plain[a, at[0], at[1]]
        for a in range(4):
            pack[0, w, pl.ds(8 + NEAR * a, 8), :] = near[a, w, pl.ds(base, 8), :]
        for a in reversed(range(4)):
            pack[1, w, pl.ds(8 + NEAR * (a - 1), 8), :] = near[a, w, pl.ds(base + rows - 8, 8), :]

    pl.semaphore_wait(barrier, neighbours)
    start_all(near_copies[4:] + near_copies[:4])
    start_all(route_copies)

    def make_masks(target, codes, w, r):
        around = {di: codes[w, pl.ds(r - di, 8), :] for di in (-1, 0, 1)}
        for k, (di, dj) in enumerate(OFFSETS):
            target[k, w, pl.ds(r, 8), :] = jnp.where(
                around[di] == jnp.float32(k + 1), jnp.float32(1.0), jnp.float32(0.0))

    def inflow(r):
        east, west, still = [], [], []
        here = pl.ds(r, 8)
        count = len(near_order)
        for w in near_order:
            x = {di: sent[w, pl.ds(r - di, 8), :] for di in (-1, 0, 1)}
            term = [near_masks[k, w, here, :] * x[di] for k, (di, _) in enumerate(OFFSETS)]
            east.append(term[0] + term[1] + term[7])
            west.append(term[3] + term[4] + term[5])
            still.append(rest[w, here, :] + term[2] + term[6])
        east = [pltpu.roll(x, 1, 1) for x in east]
        west = [pltpu.roll(x, LANES - 1, 1) for x in west]
        return [
            still[i]
            + jnp.where(lane == 0, east[i - 1], east[i])
            + jnp.where(lane == LANES - 1, west[(i + 1) % count], west[i])
            for i in range(count)
        ]

    def outflow(held, w, r):
        at = pl.ds(r, 8)
        h = held[w, at, :]
        factor = near[2, w, at, :] * jnp.exp2(jnp.log(h) * jnp.float32(2.0 / 3.0 / math.log(2.0)))
        out = h * (factor / (1.0 + factor))
        sent[w, at, :] = out
        rest[w, at, :] = h + near[1, w, at, :] - out

    for w in range(strips):
        for r in starts(base + 1, base + rows - 1):
            make_masks(near_masks, near.at[3], w, r)
        for r in range(base, base + rows, 8):
            outflow(near.at[0], w, r)

    arrive_all(near_copies)
    for r in range(0, rows, 8):
        here = pl.ds(base + r, 8)
        route[mid, pl.ds(top + r, 8), :] = jnp.where(lane < LANES // 2, near[3, right, here, :], near[3, left, here, :])
    start_all(route_mid_copies)
    for w in near_order:
        for a in range(4):
            near[a, w, pl.ds(base - 8, 8), :] = landed[0, w, pl.ds(8 + NEAR * (a - 1), 8), :]
            near[a, w, pl.ds(base + rows, 8), :] = landed[1, w, pl.ds(8 + NEAR * a, 8), :]

    reach = starts(base - NEAR, base + rows + NEAR)
    for w in near_order:
        for r in reach if w >= strips else (base - 7, base + rows - 1):
            make_masks(near_masks, near.at[3], w, r)
    for step in range(SUBSTEPS):
        for w in near_order:
            for r in (base - 8, base + rows) if step == 0 and w < strips else reach:
                outflow(near.at[0] if step == 0 else final, w, r)
        if step < SUBSTEPS - 1:
            for r in reach:
                for w, value in zip(near_order, inflow(r)):
                    final[w, pl.ds(r, 8), :] = value
    for r in range(0, rows, 8):
        new = inflow(base + r)
        for w in range(strips):
            new_depth[pl.ds(r, 8), pl.ds(w * LANES, LANES)] = new[1 + w]
            final[w, pl.ds(base + r, 8), :] = new[1 + w]
        final[mid, pl.ds(base + r, 8), :] = jnp.where(lane < LANES // 2, new[-1], new[0])

    @pl.when(me_r >= 0)
    def _():
        for r in range(0, rows, 8):
            for w, value in enumerate(to_ring([final[w, pl.ds(base + r, 8), :] for w in inner_order])):
                level[w, pl.ds(top + r, 8), :] = value
                state[0, w, pl.ds(top + r, 8), :] = value

    start_all(far_copies(level, 0))

    def ring_routes(first, last):
        for r in range(first, last, 8):
            for w, value in enumerate(to_ring([route[w, pl.ds(r, 8), :] for w in inner_order])):
                ring_route[w, pl.ds(r, 8), :] = value

    ring_routes(top, end)
    for w in inner_order:
        for r in starts(top + 1, end - 1):
            make_masks(masks, ring_route, w, r)

    def one_pass(p, blocks):
        for r in blocks:
            here = pl.ds(r, 8)
            x = {di: state[p, :, pl.ds(r - di, 8), :] for di in (-1, 0, 1)}
            term = [masks[k, :, here, :] * x[di] for k, (di, _) in enumerate(OFFSETS)]
            east = term[0] + term[1] + term[7]
            west = term[3] + term[4] + term[5]
            still = level[:, here, :] + term[2] + term[6]
            east = jnp.concatenate([pltpu.roll(east[strips:], 1, 2), east[:strips]], axis=0)
            west = jnp.concatenate([west[1:], pltpu.roll(west[:1], LANES - 1, 2)], axis=0)
            value = still + east + west
            state[p + 1, :, here, :] = value
            if p == MARGIN - 1:
                state[0, :, here, :] = value

    def halo(seg, half):
        first = end if half else top - MARGIN
        for w in inner_order:
            for r in range(0, MARGIN, 8):
                state[0, w, pl.ds(first + r, 8), :] = far[seg, half, w, pl.ds(r, 8), :]

        @pl.when(seg == 0)
        def _():
            for w in inner_order:
                for r in range(0, MARGIN, 8):
                    level[w, pl.ds(first + r, 8), :] = far[0, half, w, pl.ds(r, 8), :]

    def bands():
        for p in range(MARGIN):
            one_pass(p, starts(top - MARGIN + p + 1, top + p + 1) + starts(end - p - 1, end + MARGIN - p - 1))

    def segment(seg, carry):
        for p in range(rows // 2 - 1):
            here, stop = top + p + 1, end - p - 1
            one_pass(p, starts(here, stop) if stop - here >= 8 else [here + (stop - here) // 2 - 4])

        @pl.when(seg == 0)
        def _():
            arrive_all(route_copies)
            arrive_all(route_mid_copies)
            ring_routes(top - MARGIN, top)
            ring_routes(end, end + MARGIN)
            for w in inner_order:
                for r in (*range(top - MARGIN, top + 8, 8), *range(end - 8, end + MARGIN, 8)):
                    make_masks(masks, ring_route, w, r)

        arrive_all(far_copies(level, seg))
        leave_all(far_copies(level, seg))
        halo(seg, 0)
        halo(seg, 1)
        bands()

        @pl.when(seg == 0)
        def _():
            start_all(far_copies(state.at[MARGIN], 1))

        return carry

    lax.fori_loop(0, PASSES // MARGIN, segment, 0)

    for w in inner_order:
        for r in range(0, rows, 8):
            runoff[w, pl.ds(r, 8), :] = state[MARGIN, w, pl.ds(top + r, 8), :]
    leave_all(near_copies)
    leave_all(route_copies)
    leave_all(route_mid_copies)


def finish(level, runoff, new_depth, discharge, logs, sems):
    first = pltpu.make_async_copy(level, new_depth, sems.at[0])
    first.start()
    rows, cols = level.shape
    made = [first]
    for part in range(4):
        for r in range(part * rows // 4, (part + 1) * rows // 4, 8):
            ring = [jnp.log(1.0 + runoff[w, pl.ds(r, 8), :]) for w in range(runoff.shape[0])]
            for w in range(cols // LANES):
                logs[pl.ds(r, 8), pl.ds(w * LANES, LANES)] = from_ring(ring, w)
        at = pl.ds(part * rows // 4, rows // 4)
        made.append(pltpu.make_async_copy(logs.at[at, :], discharge.at[at, :], sems.at[1 + part]))
        made[-1].start()
    for copy in made:
        copy.wait()


def solution(mesh):
    nrow, ncol = mesh.shape["row"], mesh.shape["col"]

    def on_device(depth, rainfall, conveyance, flow_dir, outlet):
        rows, cols = depth.shape
        strips = cols // LANES
        high = rows + 2 * MARGIN + 24
        low = rows + 40
        f32 = functools.partial(pltpu.VMEM, dtype=jnp.float32)
        dma = pltpu.SemaphoreType.DMA
        segments = PASSES // MARGIN
        pin = lambda x: pltpu.with_memory_space_constraint(x, pltpu.HBM)
        depth, rainfall, conveyance, flow_dir, outlet = map(pin, (depth, rainfall, conveyance, flow_dir, outlet))
        level, runoff = pl.pallas_call(
            functools.partial(kernel, rows, cols, nrow, ncol),
            out_shape=[
                jax.ShapeDtypeStruct((rows, cols), jnp.float32),
                jax.ShapeDtypeStruct((strips + 1, rows, LANES), jnp.float32),
            ],
            in_specs=[pl.BlockSpec(memory_space=pl.ANY)] * 5,
            out_specs=[pl.BlockSpec(memory_space=pltpu.VMEM)] * 2,
            scratch_shapes=[
                f32((4, strips + 3, low, LANES)),
                f32((3, rows, cols)),
                pltpu.VMEM((rows, cols), jnp.int32),
                pltpu.VMEM((rows, cols), jnp.int32),
                f32((2, strips, 32, LANES)),
                f32((2, strips + 3, 32, LANES)),
                f32((strips + 1, high, LANES)),
                f32((strips + 1, high, LANES)),
                f32((strips + 1, high, LANES)),
                f32((strips + 3, low, LANES)),
                f32((strips + 3, low, LANES)),
                f32((8, strips + 3, low, LANES)),
                f32((8, strips + 1, high, LANES)),
                f32((MARGIN + 1, strips + 1, high, LANES)),
                f32((segments, 2, strips + 1, MARGIN, LANES)),
                f32((strips + 3, low, LANES)),
                dma((5,)),
                dma((8,)), dma((8,)), dma((2, 2)), dma((2, 2)),
                dma((segments, 2)), dma((segments, 2)),
            ],
            compiler_params=pltpu.CompilerParams(
                collective_id=0, has_side_effects=True, vmem_limit_bytes=32 * 2**20),
            name="overland",
        )(depth, rainfall, conveyance, flow_dir, outlet)
        return tuple(pl.pallas_call(
            finish,
            out_shape=[jax.ShapeDtypeStruct((rows, cols), jnp.float32)] * 2,
            in_specs=[pl.BlockSpec(memory_space=pltpu.VMEM)] * 2,
            out_specs=[pl.BlockSpec(memory_space=pl.ANY)] * 2,
            scratch_shapes=[f32((rows, cols)), dma((5,))],
            compiler_params=pltpu.CompilerParams(vmem_limit_bytes=4 * 2**20),
            name="finish",
        )(level, runoff))

    placed = P("row", "col")
    return jax.shard_map(
        on_device, mesh=mesh, in_specs=(placed,) * 5, out_specs=(placed, placed), check_vma=False)
```

```python
import functools
import math

import jax
import jax.numpy as jnp
from jax import lax
from jax.experimental import pallas as pl
from jax.experimental.pallas import tpu as pltpu
from jax.sharding import PartitionSpec as P

SUBSTEPS = 3
PASSES = 64
MARGIN = 32
HALF = MARGIN // 2
LAG = 8
LANES = 128
NEAR = 4
MESH = pl.DeviceIdType.MESH
OFFSETS = ((0, 1), (1, 1), (1, 0), (1, -1), (0, -1), (-1, -1), (-1, 0), (-1, 1))
SIDES = ((-1, 0), (1, 0), (0, -1), (0, 1), (-1, -1), (-1, 1), (1, -1), (1, 1))
VERTICAL = ((-1, 0), (1, 0))


def starts(first, last):
    made = list(range(first, last - 7, 8))
    if made[-1] + 8 < last:
        made.append(last - 8)
    return made


def to_ring(values):
    count = len(values)
    lane = lax.broadcasted_iota(jnp.int32, values[0].shape, 1)
    made = []
    for w in range(count):
        n = count * lane + w
        at = n & (LANES - 1)
        out = jnp.take_along_axis(values[0], at, axis=1)
        for k in range(1, count):
            out = jnp.where(n >= k * LANES, jnp.take_along_axis(values[k], at, axis=1), out)
        made.append(out)
    return made


def from_ring(values, strip):
    count = len(values)
    n = lax.broadcasted_iota(jnp.int32, values[0].shape, 1) + strip * LANES
    at = (n * ((1 << 18) // count + 1)) >> 18
    which = n - count * at
    out = jnp.take_along_axis(values[0], at, axis=1)
    for k in range(1, count):
        out = jnp.where(which == k, jnp.take_along_axis(values[k], at, axis=1), out)
    return out


def kernel(
    rows, cols, nrow, ncol,
    depth, rainfall, conveyance, flow_dir, outlet, new_depth, runoff,
    near, plain, flow, out_of, pack, landed, route, ring_route, level, sent, rest, near_masks, masks, state, far, final,
    in_sem, near_ssem, near_rsem, route_ssem, route_rsem, far_ssem, far_rsem,
):
    strips = cols // LANES
    mid, left, right = strips, strips + 1, strips + 2
    inner_order = list(range(strips)) + [mid]
    near_order = [left] + list(range(strips)) + [right]
    top = MARGIN + 8
    end = top + rows
    base = 16
    me_r, me_c = lax.axis_index("row"), lax.axis_index("col")
    lane = lax.broadcasted_iota(jnp.int32, (8, LANES), 1)
    zero = jnp.zeros((8, LANES), jnp.float32)
    own = pl.ds(base, rows)

    def present(dr, dc):
        r, c = me_r + dr, me_c + dc
        return (r >= 0) & (r < nrow) & (c >= 0) & (c < ncol)

    barrier = pltpu.get_barrier_semaphore()
    neighbours = jnp.int32(0)
    for dr, dc in SIDES:
        here = present(dr, dc)
        neighbours = neighbours + here.astype(jnp.int32)

        @pl.when(here)
        def _():
            pl.semaphore_signal(barrier, inc=1, device_id=(me_r + dr, me_c + dc), device_id_type=MESH)

    loads = [
        pltpu.make_async_copy(source, target, in_sem.at[a])
        for a, (source, target) in enumerate((
            (flow_dir, flow), (outlet, out_of), (conveyance, plain.at[2]), (depth, plain.at[0]), (rainfall, plain.at[1]),
        ))
    ]
    for load in loads:
        load.start()

    def clear(ref, first, last):
        for r in range(first, last, 8):
            ref[pl.ds(r, 8), :] = zero

    for half, dr in enumerate((-1, 1)):
        @pl.when(jnp.logical_not(present(dr, 0)))
        def _():
            for seg in range(PASSES // MARGIN):
                for w in inner_order:
                    clear(far.at[seg, half, w], 0, MARGIN)
            for w in range(strips):
                clear(landed.at[half, w], 8, 8 + 4 * NEAR)
            for w in inner_order:
                first = end if half else top - MARGIN
                clear(route.at[w], first, first + MARGIN)

        for w, dc in ((left, -1), (right, 1)):
            @pl.when(jnp.logical_not(present(dr, dc)))
            def _():
                clear(landed.at[half, w], 8, 8 + 4 * NEAR)

    for w, dc in ((left, -1), (right, 1)):
        @pl.when(jnp.logical_not(present(0, dc)))
        def _():
            for a in range(4):
                clear(near.at[a, w], base, base + rows)

    def remote(side, src, dst, ssem, rsem):
        return side, pltpu.make_async_remote_copy(
            src_ref=src, dst_ref=dst, send_sem=ssem, recv_sem=rsem,
            device_id=(me_r + side[0], me_c + side[1]), device_id_type=MESH)

    def start_all(made):
        for (dr, dc), copy in made:
            pl.when(present(dr, dc))(lambda: copy.start())

    def arrive_all(made):
        for (dr, dc), copy in made:
            pl.when(present(-dr, -dc))(lambda: copy.wait_recv())

    def leave_all(made):
        for (dr, dc), copy in made:
            pl.when(present(dr, dc))(lambda: copy.wait_send())

    near_copies = []
    for d, (dr, dc) in enumerate(SIDES):
        if dr == 0:
            src = near.at[:, 0 if dc < 0 else strips - 1, own, :]
            dst = near.at[:, right if dc < 0 else left, own, :]
        else:
            half, at = (0 if dr < 0 else 1), pl.ds(8, 4 * NEAR)
            if dc == 0:
                src, dst = pack.at[half, :, at, :], landed.at[1 - half, pl.ds(0, strips), at, :]
            else:
                src = pack.at[half, 0 if dc < 0 else strips - 1, at, :]
                dst = landed.at[1 - half, right if dc < 0 else left, at, :]
        near_copies.append(remote((dr, dc), src, dst, near_ssem.at[d], near_rsem.at[d]))

    edge = {-1: (pl.ds(top, MARGIN), pl.ds(end, MARGIN)), 1: (pl.ds(end - MARGIN, MARGIN), pl.ds(top - MARGIN, MARGIN))}
    route_copies, route_mid_copies = [], []
    for d, (dr, dc) in enumerate(VERTICAL):
        source, target = edge[dr]
        route_copies.append(remote(
            (dr, dc), route.at[pl.ds(0, strips), source, :], route.at[pl.ds(0, strips), target, :],
            route_ssem.at[0, d], route_rsem.at[0, d]))
        route_mid_copies.append(remote(
            (dr, dc), route.at[mid, source, :], route.at[mid, target, :], route_ssem.at[1, d], route_rsem.at[1, d]))

    def far_copies(source, seg, part):
        made = []
        for d, (dr, dc) in enumerate(VERTICAL):
            at = part * HALF if dr < 0 else (1 - part) * HALF
            made.append(remote(
                (dr, dc), source.at[:, pl.ds(at + (top if dr < 0 else end - MARGIN), HALF), :],
                far.at[seg, 1 - d, :, pl.ds(at, HALF), :],
                far_ssem.at[seg, 2 * part + d], far_rsem.at[seg, 2 * part + d]))
        return made

    for load in loads:
        load.wait()
    for w in range(strips):
        for r in range(0, rows, 8):
            at, here = (pl.ds(r, 8), pl.ds(w * LANES, LANES)), pl.ds(base + r, 8)
            code = flow[at]
            kind = jnp.where(out_of[at] == 1, 0, code + 1).astype(jnp.float32)
            near[3, w, here, :] = kind
            route[w, pl.ds(top + r, 8), :] = kind
            length = jnp.where(code % 2 == 1, jnp.float32(0.70710678), jnp.float32(1.0))
            near[2, w, here, :] = plain[2, at[0], at[1]] * length
            for a in range(2):
                near[a, w, here, :] = plain[a, at[0], at[1]]
        for a in range(4):
            pack[0, w, pl.ds(8 + NEAR * a, 8), :] = near[a, w, pl.ds(base, 8), :]
        for a in reversed(range(4)):
            pack[1, w, pl.ds(8 + NEAR * (a - 1), 8), :] = near[a, w, pl.ds(base + rows - 8, 8), :]

    pl.semaphore_wait(barrier, neighbours)
    start_all(near_copies[4:] + near_copies[:4])
    start_all(route_copies)

    def make_masks(target, codes, w, r):
        around = {di: codes[w, pl.ds(r - di, 8), :] for di in (-1, 0, 1)}
        for k, (di, dj) in enumerate(OFFSETS):
            target[k, w, pl.ds(r, 8), :] = jnp.where(
                around[di] == jnp.float32(k + 1), jnp.float32(1.0), jnp.float32(0.0))

    def inflow(r):
        east, west, still = [], [], []
        here = pl.ds(r, 8)
        count = len(near_order)
        for w in near_order:
            x = {di: sent[w, pl.ds(r - di, 8), :] for di in (-1, 0, 1)}
            term = [near_masks[k, w, here, :] * x[di] for k, (di, _) in enumerate(OFFSETS)]
            east.append(term[0] + term[1] + term[7])
            west.append(term[3] + term[4] + term[5])
            still.append(rest[w, here, :] + term[2] + term[6])
        east = [pltpu.roll(x, 1, 1) for x in east]
        west = [pltpu.roll(x, LANES - 1, 1) for x in west]
        return [
            still[i]
            + jnp.where(lane == 0, east[i - 1], east[i])
            + jnp.where(lane == LANES - 1, west[(i + 1) % count], west[i])
            for i in range(count)
        ]

    def outflow(held, w, r):
        at = pl.ds(r, 8)
        h = held[w, at, :]
        factor = near[2, w, at, :] * jnp.exp2(jnp.log(h) * jnp.float32(2.0 / 3.0 / math.log(2.0)))
        out = h * (factor / (1.0 + factor))
        sent[w, at, :] = out
        rest[w, at, :] = h + near[1, w, at, :] - out

    for w in range(strips):
        for r in starts(base + 1, base + rows - 1):
            make_masks(near_masks, near.at[3], w, r)
        for r in range(base, base + rows, 8):
            outflow(near.at[0], w, r)

    arrive_all(near_copies)
    for r in range(0, rows, 8):
        here = pl.ds(base + r, 8)
        route[mid, pl.ds(top + r, 8), :] = jnp.where(lane < LANES // 2, near[3, right, here, :], near[3, left, here, :])
    start_all(route_mid_copies)
    for w in near_order:
        for a in range(4):
            near[a, w, pl.ds(base - 8, 8), :] = landed[0, w, pl.ds(8 + NEAR * (a - 1), 8), :]
            near[a, w, pl.ds(base + rows, 8), :] = landed[1, w, pl.ds(8 + NEAR * a, 8), :]

    reach = starts(base - NEAR, base + rows + NEAR)
    for w in near_order:
        for r in reach if w >= strips else (base - 7, base + rows - 1):
            make_masks(near_masks, near.at[3], w, r)
    for step in range(SUBSTEPS):
        for w in near_order:
            for r in (base - 8, base + rows) if step == 0 and w < strips else reach:
                outflow(near.at[0] if step == 0 else final, w, r)
        if step < SUBSTEPS - 1:
            for r in reach:
                for w, value in zip(near_order, inflow(r)):
                    final[w, pl.ds(r, 8), :] = value
    for r in range(0, rows, 8):
        new = inflow(base + r)
        for w in range(strips):
            new_depth[pl.ds(r, 8), pl.ds(w * LANES, LANES)] = new[1 + w]
            final[w, pl.ds(base + r, 8), :] = new[1 + w]
        final[mid, pl.ds(base + r, 8), :] = jnp.where(lane < LANES // 2, new[-1], new[0])

    @pl.when(me_r >= 0)
    def _():
        for r in range(0, rows, 8):
            for w, value in enumerate(to_ring([final[w, pl.ds(base + r, 8), :] for w in inner_order])):
                level[w, pl.ds(top + r, 8), :] = value
                state[0, w, pl.ds(top + r, 8), :] = value

    start_all(far_copies(level, 0, 0))
    start_all(far_copies(level, 0, 1))

    def ring_routes(first, last):
        for r in range(first, last, 8):
            for w, value in enumerate(to_ring([route[w, pl.ds(r, 8), :] for w in inner_order])):
                ring_route[w, pl.ds(r, 8), :] = value

    ring_routes(top, end)
    for w in inner_order:
        for r in starts(top + 1, end - 1):
            make_masks(masks, ring_route, w, r)

    def one_pass(p, blocks):
        for r in blocks:
            here = pl.ds(r, 8)
            x = {di: state[p, :, pl.ds(r - di, 8), :] for di in (-1, 0, 1)}
            term = [masks[k, :, here, :] * x[di] for k, (di, _) in enumerate(OFFSETS)]
            east = term[0] + term[1] + term[7]
            west = term[3] + term[4] + term[5]
            still = level[:, here, :] + term[2] + term[6]
            east = jnp.concatenate([pltpu.roll(east[strips:], 1, 2), east[:strips]], axis=0)
            west = jnp.concatenate([west[1:], pltpu.roll(west[:1], LANES - 1, 2)], axis=0)
            value = still + east + west
            state[p + 1, :, here, :] = value
            if p == MARGIN - 1:
                state[0, :, here, :] = value

    def receive(seg, part):
        arrive_all(far_copies(level, seg, part))
        for half in range(2):
            at = part * HALF if half else (1 - part) * HALF
            first = end if half else top - MARGIN
            for r in range(at, at + HALF, 8):
                for w in inner_order:
                    state[0, w, pl.ds(first + r, 8), :] = far[seg, half, w, pl.ds(r, 8), :]
                    if seg == 0:
                        level[w, pl.ds(first + r, 8), :] = far[seg, half, w, pl.ds(r, 8), :]

    def inner(p):
        return starts(top - HALF + p + 1, top + p + 1) + starts(end - p - 1, end + HALF - p - 1)

    def outer(p):
        return (starts(top - MARGIN + p + 1, top - HALF + p + 1)
                + starts(end + HALF - p - 1, end + MARGIN - p - 1))

    def segment(seg, carry):
        for p in range(rows // 2 - 1):
            here, stop = top + p + 1, end - p - 1
            one_pass(p, starts(here, stop) if stop - here >= 8 else [here + (stop - here) // 2 - 4])

        @pl.when(seg == 0)
        def _():
            arrive_all(route_copies)
            arrive_all(route_mid_copies)
            ring_routes(top - MARGIN, top)
            ring_routes(end, end + MARGIN)
            for w in inner_order:
                for r in (*range(top - MARGIN, top + 8, 8), *range(end - 8, end + MARGIN, 8)):
                    make_masks(masks, ring_route, w, r)
            receive(0, 0)
            for p in range(MARGIN + LAG):
                if p == LAG:
                    receive(0, 1)
                if p < MARGIN:
                    one_pass(p, inner(p))
                if p >= LAG:
                    one_pass(p - LAG, outer(p - LAG))
                if p == MARGIN - 1:
                    start_all(far_copies(state.at[MARGIN], 1, 1))
            start_all(far_copies(state.at[MARGIN], 1, 0))
            for part in range(2):
                leave_all(far_copies(level, 0, part))

        @pl.when(seg == 1)
        def _():
            receive(1, 1)
            receive(1, 0)
            for part in range(2):
                leave_all(far_copies(level, 1, part))
            for p in range(MARGIN):
                one_pass(p, inner(p) + outer(p))

        return carry

    lax.fori_loop(0, PASSES // MARGIN, segment, 0)

    for w in inner_order:
        for r in range(0, rows, 8):
            runoff[w, pl.ds(r, 8), :] = state[MARGIN, w, pl.ds(top + r, 8), :]
    leave_all(near_copies)
    leave_all(route_copies)
    leave_all(route_mid_copies)


def finish(level, runoff, new_depth, discharge, logs, sems):
    first = pltpu.make_async_copy(level, new_depth, sems.at[0])
    first.start()
    rows, cols = level.shape
    made = [first]
    for part in range(4):
        for r in range(part * rows // 4, (part + 1) * rows // 4, 8):
            ring = [jnp.log(1.0 + runoff[w, pl.ds(r, 8), :]) for w in range(runoff.shape[0])]
            for w in range(cols // LANES):
                logs[pl.ds(r, 8), pl.ds(w * LANES, LANES)] = from_ring(ring, w)
        at = pl.ds(part * rows // 4, rows // 4)
        made.append(pltpu.make_async_copy(logs.at[at, :], discharge.at[at, :], sems.at[1 + part]))
        made[-1].start()
    for copy in made:
        copy.wait()


def solution(mesh):
    nrow, ncol = mesh.shape["row"], mesh.shape["col"]

    def on_device(depth, rainfall, conveyance, flow_dir, outlet):
        rows, cols = depth.shape
        strips = cols // LANES
        high = rows + 2 * MARGIN + 24
        low = rows + 40
        f32 = functools.partial(pltpu.VMEM, dtype=jnp.float32)
        dma = pltpu.SemaphoreType.DMA
        segments = PASSES // MARGIN
        pin = lambda x: pltpu.with_memory_space_constraint(x, pltpu.HBM)
        depth, rainfall, conveyance, flow_dir, outlet = map(pin, (depth, rainfall, conveyance, flow_dir, outlet))
        level, runoff = pl.pallas_call(
            functools.partial(kernel, rows, cols, nrow, ncol),
            out_shape=[
                jax.ShapeDtypeStruct((rows, cols), jnp.float32),
                jax.ShapeDtypeStruct((strips + 1, rows, LANES), jnp.float32),
            ],
            in_specs=[pl.BlockSpec(memory_space=pl.ANY)] * 5,
            out_specs=[pl.BlockSpec(memory_space=pltpu.VMEM)] * 2,
            scratch_shapes=[
                f32((4, strips + 3, low, LANES)),
                f32((3, rows, cols)),
                pltpu.VMEM((rows, cols), jnp.int32),
                pltpu.VMEM((rows, cols), jnp.int32),
                f32((2, strips, 32, LANES)),
                f32((2, strips + 3, 32, LANES)),
                f32((strips + 1, high, LANES)),
                f32((strips + 1, high, LANES)),
                f32((strips + 1, high, LANES)),
                f32((strips + 3, low, LANES)),
                f32((strips + 3, low, LANES)),
                f32((8, strips + 3, low, LANES)),
                f32((8, strips + 1, high, LANES)),
                f32((MARGIN + 1, strips + 1, high, LANES)),
                f32((segments, 2, strips + 1, MARGIN, LANES)),
                f32((strips + 3, low, LANES)),
                dma((5,)),
                dma((8,)), dma((8,)), dma((2, 2)), dma((2, 2)),
                dma((segments, 4)), dma((segments, 4)),
            ],
            compiler_params=pltpu.CompilerParams(
                collective_id=0, has_side_effects=True, vmem_limit_bytes=32 * 2**20),
            name="overland",
        )(depth, rainfall, conveyance, flow_dir, outlet)
        return tuple(pl.pallas_call(
            finish,
            out_shape=[jax.ShapeDtypeStruct((rows, cols), jnp.float32)] * 2,
            in_specs=[pl.BlockSpec(memory_space=pltpu.VMEM)] * 2,
            out_specs=[pl.BlockSpec(memory_space=pl.ANY)] * 2,
            scratch_shapes=[f32((rows, cols)), dma((5,))],
            compiler_params=pltpu.CompilerParams(vmem_limit_bytes=4 * 2**20),
            name="finish",
        )(level, runoff))

    placed = P("row", "col")
    return jax.shard_map(
        on_device, mesh=mesh, in_specs=(placed,) * 5, out_specs=(placed, placed), check_vma=False)
```

```python
import functools
import math

import jax
import jax.numpy as jnp
from jax import lax
from jax.experimental import pallas as pl
from jax.experimental.pallas import tpu as pltpu
from jax.sharding import PartitionSpec as P

SUBSTEPS = 3
PASSES = 64
MARGIN = 32
HALF = MARGIN // 2
LAG = 8
LANES = 128
NEAR = 4
MESH = pl.DeviceIdType.MESH
OFFSETS = ((0, 1), (1, 1), (1, 0), (1, -1), (0, -1), (-1, -1), (-1, 0), (-1, 1))
SIDES = ((-1, 0), (1, 0), (0, -1), (0, 1), (-1, -1), (-1, 1), (1, -1), (1, 1))
VERTICAL = ((-1, 0), (1, 0))


def starts(first, last):
    made = list(range(first, last - 7, 8))
    if made[-1] + 8 < last:
        made.append(last - 8)
    return made


def to_ring(values):
    count = len(values)
    lane = lax.broadcasted_iota(jnp.int32, values[0].shape, 1)
    made = []
    for w in range(count):
        n = count * lane + w
        at = n & (LANES - 1)
        out = jnp.take_along_axis(values[0], at, axis=1)
        for k in range(1, count):
            out = jnp.where(n >= k * LANES, jnp.take_along_axis(values[k], at, axis=1), out)
        made.append(out)
    return made


def from_ring(values, strip):
    count = len(values)
    n = lax.broadcasted_iota(jnp.int32, values[0].shape, 1) + strip * LANES
    at = (n * ((1 << 18) // count + 1)) >> 18
    which = n - count * at
    out = jnp.take_along_axis(values[0], at, axis=1)
    for k in range(1, count):
        out = jnp.where(which == k, jnp.take_along_axis(values[k], at, axis=1), out)
    return out


def kernel(
    rows, cols, nrow, ncol,
    depth, rainfall, conveyance, flow_dir, outlet, new_depth, runoff,
    near, plain, flow, out_of, pack, landed, route, ring_route, level, sent, rest, near_masks, masks, state, far, final,
    in_sem, near_ssem, near_rsem, route_ssem, route_rsem, far_ssem, far_rsem,
):
    strips = cols // LANES
    mid, left, right = strips, strips + 1, strips + 2
    inner_order = list(range(strips)) + [mid]
    near_order = [left] + list(range(strips)) + [right]
    top = MARGIN + 8
    end = top + rows
    base = 16
    me_r, me_c = lax.axis_index("row"), lax.axis_index("col")
    lane = lax.broadcasted_iota(jnp.int32, (8, LANES), 1)
    zero = jnp.zeros((8, LANES), jnp.float32)
    own = pl.ds(base, rows)

    def present(dr, dc):
        r, c = me_r + dr, me_c + dc
        return (r >= 0) & (r < nrow) & (c >= 0) & (c < ncol)

    barrier = pltpu.get_barrier_semaphore()
    neighbours = jnp.int32(0)
    for dr, dc in SIDES:
        here = present(dr, dc)
        neighbours = neighbours + here.astype(jnp.int32)

        @pl.when(here)
        def _():
            pl.semaphore_signal(barrier, inc=1, device_id=(me_r + dr, me_c + dc), device_id_type=MESH)

    loads = [
        pltpu.make_async_copy(source, target, in_sem.at[a])
        for a, (source, target) in enumerate((
            (flow_dir, flow), (outlet, out_of), (conveyance, plain.at[2]), (depth, plain.at[0]), (rainfall, plain.at[1]),
        ))
    ]
    for load in loads:
        load.start()

    def clear(ref, first, last):
        for r in range(first, last, 8):
            ref[pl.ds(r, 8), :] = zero

    for half, dr in enumerate((-1, 1)):
        @pl.when(jnp.logical_not(present(dr, 0)))
        def _():
            for seg in range(PASSES // MARGIN):
                for w in inner_order:
                    clear(far.at[seg, half, w], 0, MARGIN)
            for w in range(strips):
                clear(landed.at[half, w], 8, 8 + 4 * NEAR)
            for w in inner_order:
                first = end if half else top - MARGIN
                clear(route.at[w], first, first + MARGIN)

        for w, dc in ((left, -1), (right, 1)):
            @pl.when(jnp.logical_not(present(dr, dc)))
            def _():
                clear(landed.at[half, w], 8, 8 + 4 * NEAR)

    for w, dc in ((left, -1), (right, 1)):
        @pl.when(jnp.logical_not(present(0, dc)))
        def _():
            for a in range(4):
                clear(near.at[a, w], base, base + rows)

    def remote(side, src, dst, ssem, rsem):
        return side, pltpu.make_async_remote_copy(
            src_ref=src, dst_ref=dst, send_sem=ssem, recv_sem=rsem,
            device_id=(me_r + side[0], me_c + side[1]), device_id_type=MESH)

    def start_all(made):
        for (dr, dc), copy in made:
            pl.when(present(dr, dc))(lambda: copy.start())

    def arrive_all(made):
        for (dr, dc), copy in made:
            pl.when(present(-dr, -dc))(lambda: copy.wait_recv())

    def leave_all(made):
        for (dr, dc), copy in made:
            pl.when(present(dr, dc))(lambda: copy.wait_send())

    near_copies = []
    for d, (dr, dc) in enumerate(SIDES):
        if dr == 0:
            src = near.at[:, 0 if dc < 0 else strips - 1, own, :]
            dst = near.at[:, right if dc < 0 else left, own, :]
        else:
            half, at = (0 if dr < 0 else 1), pl.ds(8, 4 * NEAR)
            if dc == 0:
                src, dst = pack.at[half, :, at, :], landed.at[1 - half, pl.ds(0, strips), at, :]
            else:
                src = pack.at[half, 0 if dc < 0 else strips - 1, at, :]
                dst = landed.at[1 - half, right if dc < 0 else left, at, :]
        near_copies.append(remote((dr, dc), src, dst, near_ssem.at[d], near_rsem.at[d]))

    edge = {-1: (pl.ds(top, MARGIN), pl.ds(end, MARGIN)), 1: (pl.ds(end - MARGIN, MARGIN), pl.ds(top - MARGIN, MARGIN))}
    route_copies, route_mid_copies = [], []
    for d, (dr, dc) in enumerate(VERTICAL):
        source, target = edge[dr]
        route_copies.append(remote(
            (dr, dc), route.at[pl.ds(0, strips), source, :], route.at[pl.ds(0, strips), target, :],
            route_ssem.at[0, d], route_rsem.at[0, d]))
        route_mid_copies.append(remote(
            (dr, dc), route.at[mid, source, :], route.at[mid, target, :], route_ssem.at[1, d], route_rsem.at[1, d]))

    def far_copies(source, seg, part):
        made = []
        for d, (dr, dc) in enumerate(VERTICAL):
            at = part * HALF if dr < 0 else (1 - part) * HALF
            made.append(remote(
                (dr, dc), source.at[:, pl.ds(at + (top if dr < 0 else end - MARGIN), HALF), :],
                far.at[seg, 1 - d, :, pl.ds(at, HALF), :],
                far_ssem.at[seg, 2 * part + d], far_rsem.at[seg, 2 * part + d]))
        return made

    for load in loads:
        load.wait()
    for w in range(strips):
        for r in range(0, rows, 8):
            at, here = (pl.ds(r, 8), pl.ds(w * LANES, LANES)), pl.ds(base + r, 8)
            code = flow[at]
            kind = jnp.where(out_of[at] == 1, 0, code + 1).astype(jnp.float32)
            near[3, w, here, :] = kind
            route[w, pl.ds(top + r, 8), :] = kind
            length = jnp.where(code % 2 == 1, jnp.float32(0.70710678), jnp.float32(1.0))
            near[2, w, here, :] = plain[2, at[0], at[1]] * length
            for a in range(2):
                near[a, w, here, :] = plain[a, at[0], at[1]]
        for a in range(4):
            pack[0, w, pl.ds(8 + NEAR * a, 8), :] = near[a, w, pl.ds(base, 8), :]
        for a in reversed(range(4)):
            pack[1, w, pl.ds(8 + NEAR * (a - 1), 8), :] = near[a, w, pl.ds(base + rows - 8, 8), :]

    pl.semaphore_wait(barrier, neighbours)
    start_all(near_copies[4:] + near_copies[:4])
    start_all(route_copies)

    def make_masks(target, codes, w, r):
        around = {di: codes[w, pl.ds(r - di, 8), :] for di in (-1, 0, 1)}
        for k, (di, dj) in enumerate(OFFSETS):
            target[k, w, pl.ds(r, 8), :] = jnp.where(
                around[di] == jnp.float32(k + 1), jnp.float32(1.0), jnp.float32(0.0))

    def inflow(r):
        east, west, still = [], [], []
        here = pl.ds(r, 8)
        count = len(near_order)
        for w in near_order:
            x = {di: sent[w, pl.ds(r - di, 8), :] for di in (-1, 0, 1)}
            term = [near_masks[k, w, here, :] * x[di] for k, (di, _) in enumerate(OFFSETS)]
            east.append(term[0] + term[1] + term[7])
            west.append(term[3] + term[4] + term[5])
            still.append(rest[w, here, :] + term[2] + term[6])
        east = [pltpu.roll(x, 1, 1) for x in east]
        west = [pltpu.roll(x, LANES - 1, 1) for x in west]
        return [
            still[i]
            + jnp.where(lane == 0, east[i - 1], east[i])
            + jnp.where(lane == LANES - 1, west[(i + 1) % count], west[i])
            for i in range(count)
        ]

    def outflow(held, w, r):
        at = pl.ds(r, 8)
        h = held[w, at, :]
        factor = near[2, w, at, :] * jnp.exp2(jnp.log(h) * jnp.float32(2.0 / 3.0 / math.log(2.0)))
        out = h * (factor / (1.0 + factor))
        sent[w, at, :] = out
        rest[w, at, :] = h + near[1, w, at, :] - out

    for w in range(strips):
        for r in starts(base + 1, base + rows - 1):
            make_masks(near_masks, near.at[3], w, r)
        for r in range(base, base + rows, 8):
            outflow(near.at[0], w, r)

    arrive_all(near_copies)
    for r in range(0, rows, 8):
        here = pl.ds(base + r, 8)
        route[mid, pl.ds(top + r, 8), :] = jnp.where(lane < LANES // 2, near[3, right, here, :], near[3, left, here, :])
    start_all(route_mid_copies)
    for w in near_order:
        for a in range(4):
            near[a, w, pl.ds(base - 8, 8), :] = landed[0, w, pl.ds(8 + NEAR * (a - 1), 8), :]
            near[a, w, pl.ds(base + rows, 8), :] = landed[1, w, pl.ds(8 + NEAR * a, 8), :]

    reach = starts(base - NEAR, base + rows + NEAR)
    for w in near_order:
        for r in reach if w >= strips else (base - 7, base + rows - 1):
            make_masks(near_masks, near.at[3], w, r)
    for step in range(SUBSTEPS):
        for w in near_order:
            for r in (base - 8, base + rows) if step == 0 and w < strips else reach:
                outflow(near.at[0] if step == 0 else final, w, r)
        if step < SUBSTEPS - 1:
            for r in reach:
                for w, value in zip(near_order, inflow(r)):
                    final[w, pl.ds(r, 8), :] = value
    for r in range(0, rows, 8):
        new = inflow(base + r)
        for w in range(strips):
            new_depth[pl.ds(r, 8), pl.ds(w * LANES, LANES)] = new[1 + w]
            final[w, pl.ds(base + r, 8), :] = new[1 + w]
        final[mid, pl.ds(base + r, 8), :] = jnp.where(lane < LANES // 2, new[-1], new[0])

    for part, blocks in enumerate((
        (*range(0, HALF, 8), *range(rows - HALF, rows, 8)), range(HALF, rows - HALF, 8),
    )):
        @pl.when(me_r >= 0)
        def _():
            for r in blocks:
                for w, value in enumerate(to_ring([final[w, pl.ds(base + r, 8), :] for w in inner_order])):
                    level[w, pl.ds(top + r, 8), :] = value
                    state[0, w, pl.ds(top + r, 8), :] = value

        start_all(far_copies(level, 0, part))

    def ring_routes(first, last):
        for r in range(first, last, 8):
            for w, value in enumerate(to_ring([route[w, pl.ds(r, 8), :] for w in inner_order])):
                ring_route[w, pl.ds(r, 8), :] = value

    ring_routes(top, end)
    for w in inner_order:
        for r in starts(top + 1, end - 1):
            make_masks(masks, ring_route, w, r)

    def one_pass(p, blocks):
        for r in blocks:
            here = pl.ds(r, 8)
            x = {di: state[p, :, pl.ds(r - di, 8), :] for di in (-1, 0, 1)}
            term = [masks[k, :, here, :] * x[di] for k, (di, _) in enumerate(OFFSETS)]
            east = term[0] + term[1] + term[7]
            west = term[3] + term[4] + term[5]
            still = level[:, here, :] + term[2] + term[6]
            east = jnp.concatenate([pltpu.roll(east[strips:], 1, 2), east[:strips]], axis=0)
            west = jnp.concatenate([west[1:], pltpu.roll(west[:1], LANES - 1, 2)], axis=0)
            value = still + east + west
            state[p + 1, :, here, :] = value
            if p == MARGIN - 1:
                state[0, :, here, :] = value

    def receive(seg, part):
        arrive_all(far_copies(level, seg, part))
        for half in range(2):
            at = part * HALF if half else (1 - part) * HALF
            first = end if half else top - MARGIN
            for r in range(at, at + HALF, 8):
                for w in inner_order:
                    state[0, w, pl.ds(first + r, 8), :] = far[seg, half, w, pl.ds(r, 8), :]
                    if seg == 0:
                        level[w, pl.ds(first + r, 8), :] = far[seg, half, w, pl.ds(r, 8), :]

    def inner(p):
        return starts(top - HALF + p + 1, top + p + 1) + starts(end - p - 1, end + HALF - p - 1)

    def outer(p):
        return (starts(top - MARGIN + p + 1, top - HALF + p + 1)
                + starts(end + HALF - p - 1, end + MARGIN - p - 1))

    def segment(seg, carry):
        for p in range(rows // 2 - 1):
            here, stop = top + p + 1, end - p - 1
            one_pass(p, starts(here, stop) if stop - here >= 8 else [here + (stop - here) // 2 - 4])

        @pl.when(seg == 0)
        def _():
            arrive_all(route_copies)
            arrive_all(route_mid_copies)
            ring_routes(top - MARGIN, top)
            ring_routes(end, end + MARGIN)
            for w in inner_order:
                for r in (*range(top - MARGIN, top + 8, 8), *range(end - 8, end + MARGIN, 8)):
                    make_masks(masks, ring_route, w, r)
            receive(0, 0)
            for p in range(MARGIN + LAG):
                if p == LAG:
                    receive(0, 1)
                if p < MARGIN:
                    one_pass(p, inner(p))
                if p >= LAG:
                    one_pass(p - LAG, outer(p - LAG))
                if p == MARGIN - 1:
                    start_all(far_copies(state.at[MARGIN], 1, 1))
            start_all(far_copies(state.at[MARGIN], 1, 0))
            for part in range(2):
                leave_all(far_copies(level, 0, part))

        @pl.when(seg == 1)
        def _():
            receive(1, 1)
            receive(1, 0)
            for part in range(2):
                leave_all(far_copies(level, 1, part))
            for p in range(MARGIN):
                one_pass(p, inner(p) + outer(p))

        return carry

    lax.fori_loop(0, PASSES // MARGIN, segment, 0)

    for w in inner_order:
        for r in range(0, rows, 8):
            runoff[w, pl.ds(r, 8), :] = state[MARGIN, w, pl.ds(top + r, 8), :]
    leave_all(near_copies)
    leave_all(route_copies)
    leave_all(route_mid_copies)


def finish(level, runoff, new_depth, discharge, logs, sems):
    first = pltpu.make_async_copy(level, new_depth, sems.at[0])
    first.start()
    rows, cols = level.shape
    made = [first]
    for part in range(4):
        for r in range(part * rows // 4, (part + 1) * rows // 4, 8):
            ring = [jnp.log(1.0 + runoff[w, pl.ds(r, 8), :]) for w in range(runoff.shape[0])]
            for w in range(cols // LANES):
                logs[pl.ds(r, 8), pl.ds(w * LANES, LANES)] = from_ring(ring, w)
        at = pl.ds(part * rows // 4, rows // 4)
        made.append(pltpu.make_async_copy(logs.at[at, :], discharge.at[at, :], sems.at[1 + part]))
        made[-1].start()
    for copy in made:
        copy.wait()


def solution(mesh):
    nrow, ncol = mesh.shape["row"], mesh.shape["col"]

    def on_device(depth, rainfall, conveyance, flow_dir, outlet):
        rows, cols = depth.shape
        strips = cols // LANES
        high = rows + 2 * MARGIN + 24
        low = rows + 40
        f32 = functools.partial(pltpu.VMEM, dtype=jnp.float32)
        dma = pltpu.SemaphoreType.DMA
        segments = PASSES // MARGIN
        pin = lambda x: pltpu.with_memory_space_constraint(x, pltpu.HBM)
        depth, rainfall, conveyance, flow_dir, outlet = map(pin, (depth, rainfall, conveyance, flow_dir, outlet))
        level, runoff = pl.pallas_call(
            functools.partial(kernel, rows, cols, nrow, ncol),
            out_shape=[
                jax.ShapeDtypeStruct((rows, cols), jnp.float32),
                jax.ShapeDtypeStruct((strips + 1, rows, LANES), jnp.float32),
            ],
            in_specs=[pl.BlockSpec(memory_space=pl.ANY)] * 5,
            out_specs=[pl.BlockSpec(memory_space=pltpu.VMEM)] * 2,
            scratch_shapes=[
                f32((4, strips + 3, low, LANES)),
                f32((3, rows, cols)),
                pltpu.VMEM((rows, cols), jnp.int32),
                pltpu.VMEM((rows, cols), jnp.int32),
                f32((2, strips, 32, LANES)),
                f32((2, strips + 3, 32, LANES)),
                f32((strips + 1, high, LANES)),
                f32((strips + 1, high, LANES)),
                f32((strips + 1, high, LANES)),
                f32((strips + 3, low, LANES)),
                f32((strips + 3, low, LANES)),
                f32((8, strips + 3, low, LANES)),
                f32((8, strips + 1, high, LANES)),
                f32((MARGIN + 1, strips + 1, high, LANES)),
                f32((segments, 2, strips + 1, MARGIN, LANES)),
                f32((strips + 3, low, LANES)),
                dma((5,)),
                dma((8,)), dma((8,)), dma((2, 2)), dma((2, 2)),
                dma((segments, 4)), dma((segments, 4)),
            ],
            compiler_params=pltpu.CompilerParams(
                collective_id=0, has_side_effects=True, vmem_limit_bytes=32 * 2**20),
            name="overland",
        )(depth, rainfall, conveyance, flow_dir, outlet)
        return tuple(pl.pallas_call(
            finish,
            out_shape=[jax.ShapeDtypeStruct((rows, cols), jnp.float32)] * 2,
            in_specs=[pl.BlockSpec(memory_space=pltpu.VMEM)] * 2,
            out_specs=[pl.BlockSpec(memory_space=pl.ANY)] * 2,
            scratch_shapes=[f32((rows, cols)), dma((5,))],
            compiler_params=pltpu.CompilerParams(vmem_limit_bytes=4 * 2**20),
            name="finish",
        )(level, runoff))

    placed = P("row", "col")
    return jax.shard_map(
        on_device, mesh=mesh, in_specs=(placed,) * 5, out_specs=(placed, placed), check_vma=False)
```
